64 devices in a mesh: rep: 8 (over x, y, core), dp: 8 (over z).
Axes of the slice: x: 2, y: 2, z: 8, core: 2. Of those that a mesh axis runs over, the one named last changes fastest.
The devices are a block of a 4x4x8 slice.
Arguments:
- g_w_gate: bfloat16 [64, 2, 512, 1280], P(('rep', 'dp')), parts along dimension 0
- g_w_up: bfloat16 [64, 2, 512, 1280], P(('rep', 'dp')), parts along dimension 0
- g_w_down: bfloat16 [64, 2, 1280, 512], P(('rep', 'dp')), parts along dimension 0
- w_gate: bfloat16 [2, 512, 1280], replicated
- w_up: bfloat16 [2, 512, 1280], replicated
- w_down: bfloat16 [2, 1280, 512], replicated
- m_w_gate: float32 [2, 512, 1280], P(None, 'dp')
- m_w_up: float32 [2, 512, 1280], P(None, 'dp')
- m_w_down: float32 [2, 1280, 512], P(None, 'dp')
- v_w_gate: float32 [2, 512, 1280], P(None, 'dp')
- v_w_up: float32 [2, 512, 1280], P(None, 'dp')
- v_w_down: float32 [2, 1280, 512], P(None, 'dp')
Outputs:
- output 1: bfloat16 [16, 512, 1280], P('rep'), parts along dimension 0
- output 2: bfloat16 [16, 512, 1280], P('rep'), parts along dimension 0
- output 3: bfloat16 [16, 1280, 512], P('rep'), parts along dimension 0
- output 4: float32 [16, 512, 1280], P('rep', 'dp'), parts along dimension 0
- output 5: float32 [16, 512, 1280], P('rep', 'dp'), parts along dimension 0
- output 6: float32 [16, 1280, 512], P('rep', 'dp'), parts along dimension 0
- output 7: float32 [16, 512, 1280], P('rep', 'dp'), parts along dimension 0
- output 8: float32 [16, 512, 1280], P('rep', 'dp'), parts along dimension 0
- output 9: float32 [16, 1280, 512], P('rep', 'dp'), parts along dimension 0
There are 8 independent parts. The reference program is written for one: setup_inputs(seed, part) draws one part's arguments, and reference() takes and returns one part's arrays. A program takes and returns all parts, laid end to end along the dimension named above; an argument that names none is the same for every part.
All inputs are finite; a program needn't handle non-finite values.
Results may differ from the reference program's by a relative error of at most 0.022.
Values are sent between devices in bfloat16 or wider.
A program may use at most 768 MiB of HBM per device.

```python
import jax
import jax.numpy as jnp
from jax import lax

DEVICES = 8
D = 512
FF = 1280
LAYERS = 2
NAMES = ("w_gate", "w_up", "w_down")
SHAPES = {"w_gate": (LAYERS, D, FF), "w_up": (LAYERS, D, FF), "w_down": (LAYERS, FF, D)}


def setup_inputs(seed: int = 0, part: int = 0) -> dict:
    kz, *keys = jax.random.split(jax.random.key(seed), 1 + 5 * len(NAMES))
    loud = 2.0 ** jax.random.uniform(kz, (), jnp.float32, -1.0, 1.0)
    drawn = {}
    for name, key, both in zip(NAMES, keys[:3], keys[3:6], strict=True):
        own = jax.random.normal(jax.random.fold_in(key, part), (DEVICES, *SHAPES[name]), jnp.float32)
        shared = jax.random.normal(jax.random.fold_in(both, part), SHAPES[name], jnp.float32)
        drawn["g_" + name] = (loud * (0.7 * shared / DEVICES + 0.7 * own * DEVICES**-0.5)).astype(jnp.bfloat16)
    for name, key in zip(NAMES, keys[6:9], strict=True):
        drawn[name] = (jax.random.normal(key, SHAPES[name], jnp.float32) * SHAPES[name][1] ** -0.5).astype(jnp.bfloat16)
    for name, key in zip(NAMES, keys[9:12], strict=True):
        drawn["m_" + name] = loud * 0.5 * jax.random.normal(key, SHAPES[name], jnp.float32)
    for name, key in zip(NAMES, keys[12:15], strict=True):
        drawn["v_" + name] = loud * loud * jax.random.uniform(key, SHAPES[name], jnp.float32, 0.5, 1.5)
    return drawn


def adamw(w, m, v, g):
    m = 0.9 * m + 0.1 * g
    v = 0.95 * v + 0.05 * g * g
    step = m * lax.rsqrt(v + 1e-8) + 0.1 * w
    return (w - 0.02 * step).astype(jnp.bfloat16), m, v


def reference(g_w_gate, g_w_up, g_w_down, w_gate, w_up, w_down, m_w_gate, m_w_up, m_w_down, v_w_gate, v_w_up, v_w_down):
    def total(terms):
        return lax.scan(lambda so_far, term: (so_far + term.astype(jnp.float32), None), jnp.zeros(terms.shape[1:], jnp.float32), terms)[0]

    gradients = [total(terms).astype(jnp.bfloat16).astype(jnp.float32) for terms in (g_w_gate, g_w_up, g_w_down)]
    new = [
        adamw(w.astype(jnp.float32), m, v, g)
        for w, m, v, g in zip((w_gate, w_up, w_down), (m_w_gate, m_w_up, m_w_down), (v_w_gate, v_w_up, v_w_down), gradients, strict=True)
    ]
    return tuple(one[which] for which in range(3) for one in new)
```

```python
import functools

import jax
import jax.numpy as jnp
from jax import lax
from jax.experimental import pallas as pl
from jax.experimental.pallas import tpu as pltpu
from jax.sharding import PartitionSpec as P

AXIS = "dp"
PARTS = 2


def adamw(w, m, v, g):
    m = 0.9 * m + 0.1 * g
    v = 0.95 * v + 0.05 * g * g
    step = m * lax.rsqrt(v + 1e-8) + 0.1 * w
    return (w - 0.02 * step).astype(jnp.bfloat16), m, v


def kernel(n, *refs):
    terms, weights, ms, vs = (refs[i : i + 3] for i in (0, 3, 6, 9))
    new_w, new_m, new_v = (refs[i : i + 3] for i in (12, 15, 18))
    held, sums, own = (refs[i : i + 3] for i in (21, 24, 27))
    held_sem, own_sem, m_sem, v_sem, sum_send, sum_recv, out_send, out_recv = refs[30:]
    layers = held[0].shape[0]
    me = lax.axis_index(AXIS)
    right, left = lax.rem(me + 1, n), lax.rem(me + n - 1, n)
    every = [(i, layer) for i in range(3) for layer in range(layers)]
    pieces = [
        (i, layer, part * (sums[i].shape[2] // PARTS), sums[i].shape[2] // PARTS)
        for i in range(3)
        for part in range(PARTS)
        for half in range(layers // 2)
        for layer in (half, half + layers // 2)
    ]

    def rightward(layer):
        return layer < layers // 2

    def to(layer):
        return {AXIS: right if rightward(layer) else left}

    def behind(layer, k):
        return lax.rem(me + n - k if rightward(layer) else me + k, n)

    def rows(i, block, first, count):
        return pl.ds(pl.multiple_of(block * sums[i].shape[2] + first, 16), count)

    def load(i, layer, k):
        block = rows(i, behind(layer, k), 0, sums[i].shape[2])
        return pltpu.make_async_copy(terms[i].at[0, layer, block], held[i].at[layer, block], held_sem.at[i, layer, k - 1])

    def sum_copy(at, step, source):
        i, layer, first, count = pieces[at]
        return pltpu.make_async_remote_copy(
            src_ref=source,
            dst_ref=sums[i].at[layer, step, pl.ds(first, count)],
            send_sem=sum_send.at[step, at],
            recv_sem=sum_recv.at[step, at],
            device_id=to(layer),
            device_id_type=pl.DeviceIdType.MESH,
        )

    def out_copy(at, step):
        i, layer, first, count = pieces[at]
        piece = new_w[i].at[layer, rows(i, behind(layer, step), first, count)]
        return pltpu.make_async_remote_copy(
            src_ref=piece,
            dst_ref=piece,
            send_sem=out_send.at[step, at],
            recv_sem=out_recv.at[step, at],
            device_id=to(layer),
            device_id_type=pl.DeviceIdType.MESH,
        )

    def landed(at, step):
        i, layer, first, count = pieces[at]
        return sums[i].at[layer, step, pl.ds(first, count)]

    def term(at, k):
        i, layer, first, count = pieces[at]
        return held[i].at[layer, rows(i, behind(layer, k), first, count)]

    def own_load(i, layer):
        return pltpu.make_async_copy(weights[i].at[layer, rows(i, me, 0, sums[i].shape[2])], own[i].at[layer], own_sem.at[i, layer])

    def moment_load(i):
        return (pltpu.make_async_copy(ms[i], new_m[i], m_sem.at[i]), pltpu.make_async_copy(vs[i], new_v[i], v_sem.at[i]))

    barrier = pltpu.get_barrier_semaphore()
    for neighbour in (left, right):
        pl.semaphore_signal(barrier, inc=1, device_id={AXIS: neighbour}, device_id_type=pl.DeviceIdType.MESH)
    for k in range(1, n + 1):
        for i, layer in every:
            load(i, layer, k).start()
    for i, layer in every:
        own_load(i, layer).start()
    for i in range(3):
        for copy in moment_load(i):
            copy.start()
    pl.semaphore_wait(barrier, 2)

    for at, (i, layer, first, count) in enumerate(pieces):
        if first == 0:
            load(i, layer, 1).wait()
        sum_copy(at, 0, term(at, 1)).start()

    @pl.loop(0, n - 2)
    def _(step):
        for at, (i, layer, first, count) in enumerate(pieces):
            here = landed(at, step)
            sum_copy(at, step, here).wait_recv()
            if first == 0:
                load(i, layer, step + 2).wait()
            here[...] = (here[...].astype(jnp.float32) + term(at, step + 2)[...].astype(jnp.float32)).astype(jnp.bfloat16)
            sum_copy(at, step + 1, here).start()

    for i, layer in every:
        own_load(i, layer).wait()
    for i in range(3):
        for copy in moment_load(i):
            copy.wait()

    for at, (i, layer, first, count) in enumerate(pieces):
        here = landed(at, n - 2)
        sum_copy(at, n - 2, here).wait_recv()
        if first == 0:
            load(i, layer, n).wait()
        g = (here[...].astype(jnp.float32) + term(at, n)[...].astype(jnp.float32)).astype(jnp.bfloat16).astype(jnp.float32)
        piece = (layer, pl.ds(first, count))
        w, m, v = adamw(own[i][piece].astype(jnp.float32), new_m[i][piece], new_v[i][piece], g)
        new_w[i][layer, rows(i, me, first, count)] = w
        new_m[i][piece] = m
        new_v[i][piece] = v
        out_copy(at, 0).start()

    @pl.loop(0, n - 2)
    def _(step):
        for at in range(len(pieces)):
            out_copy(at, step).wait_recv()
            out_copy(at, step + 1).start()

    for at in range(len(pieces)):
        out_copy(at, n - 2).wait_recv()

    @pl.loop(0, n - 1)
    def _(step):
        for at in range(len(pieces)):
            sum_copy(at, step, landed(at, step)).wait_send()
            out_copy(at, step).wait_send()


def put(*refs):
    count = len(refs) // 2
    copies = [pltpu.make_async_copy(refs[i], refs[count + i], refs[-1].at[i]) for i in range(count)]
    for copy in copies:
        copy.start()
    for copy in copies:
        copy.wait()


def solution(mesh):
    n = mesh.shape[AXIS]

    def step(*arrays):
        terms, weights, m, v = (arrays[i : i + 3] for i in (0, 3, 6, 9))
        layers = m[0].shape[0]
        count = 3 * layers * PARTS
        dma = pltpu.SemaphoreType.DMA
        arrays = [pltpu.with_memory_space_constraint(one, pltpu.HBM) for one in arrays]
        new = pl.pallas_call(
            functools.partial(kernel, n),
            out_shape=tuple(pltpu.VMEM(w.shape, w.dtype) for w in weights) + tuple(pltpu.VMEM(one.shape, one.dtype) for one in m + v),
            in_specs=[pl.BlockSpec(memory_space=pltpu.HBM)] * 12,
            out_specs=(pl.BlockSpec(memory_space=pltpu.VMEM),) * 9,
            scratch_shapes=[pltpu.VMEM(w.shape, w.dtype) for w in weights]
            + [pltpu.VMEM((layers, n - 1, *one.shape[1:]), w.dtype) for w, one in zip(weights, m, strict=True)]
            + [pltpu.VMEM(one.shape, w.dtype) for w, one in zip(weights, m, strict=True)]
            + [dma((3, layers, n)), dma((3, layers)), dma((3,)), dma((3,))]
            + [dma((n - 1, count))] * 4,
            compiler_params=pltpu.CompilerParams(collective_id=0, has_side_effects=True, vmem_limit_bytes=40 * 2**20),
        )(*arrays)
        new = [pltpu.with_memory_space_constraint(one, pltpu.VMEM) for one in new]
        return pl.pallas_call(
            put,
            out_shape=tuple(pltpu.HBM(one.shape, one.dtype) for one in new),
            in_specs=[pl.BlockSpec(memory_space=pltpu.VMEM)] * 9,
            out_specs=(pl.BlockSpec(memory_space=pltpu.HBM),) * 9,
            scratch_shapes=[dma((9,))],
            compiler_params=pltpu.CompilerParams(vmem_limit_bytes=2**20),
        )(*new)

    all_of, cut = P(None, None, None), P(None, AXIS, None)
    return jax.shard_map(
        step,
        mesh=mesh,
        in_specs=(P(("rep", AXIS), None, None, None),) * 3 + (all_of,) * 3 + (cut,) * 6,
        out_specs=(P("rep", None, None),) * 3 + (P("rep", AXIS, None),) * 6,
        check_vma=False,
    )
```

```python
import functools

import jax
import jax.numpy as jnp
from jax import lax
from jax.experimental import pallas as pl
from jax.experimental.pallas import tpu as pltpu
from jax.sharding import PartitionSpec as P

AXIS = "dp"
PARTS = 2


def adamw(w, m, v, g):
    m = 0.9 * m + 0.1 * g
    v = 0.95 * v + 0.05 * g * g
    step = m * lax.rsqrt(v + 1e-8) + 0.1 * w
    return (w - 0.02 * step).astype(jnp.bfloat16), m, v


def kernel(n, *refs):
    terms, weights, ms, vs = (refs[i : i + 3] for i in (0, 3, 6, 9))
    new_w, new_m, new_v = (refs[i : i + 3] for i in (12, 15, 18))
    held, sums, own = (refs[i : i + 3] for i in (21, 24, 27))
    held_sem, own_sem, m_sem, v_sem, sum_send, sum_recv, out_send, out_recv = refs[30:]
    layers = held[0].shape[0]
    me = lax.axis_index(AXIS)
    right, left = lax.rem(me + 1, n), lax.rem(me + n - 1, n)
    every = [(i, layer) for i in range(3) for layer in range(layers)]
    pieces = [
        (i, layer, part * (sums[i].shape[2] // PARTS), sums[i].shape[2] // PARTS)
        for i in range(3)
        for part in range(PARTS)
        for half in range(layers // 2)
        for layer in (half, half + layers // 2)
    ]

    def rightward(layer):
        return layer < layers // 2

    def to(layer):
        return {AXIS: right if rightward(layer) else left}

    def behind(layer, k):
        return lax.rem(me + n - k if rightward(layer) else me + k, n)

    def rows(i, block, first, count):
        return pl.ds(pl.multiple_of(block * sums[i].shape[2] + first, 16), count)

    def load(i, layer, k):
        block = rows(i, behind(layer, k), 0, sums[i].shape[2])
        return pltpu.make_async_copy(terms[i].at[0, layer, block], held[i].at[layer, block], held_sem.at[i, layer, k - 2])

    def sum_copy(at, step, source):
        i, layer, first, count = pieces[at]
        return pltpu.make_async_remote_copy(
            src_ref=source,
            dst_ref=sums[i].at[layer, step, pl.ds(first, count)],
            send_sem=sum_send.at[step, at],
            recv_sem=sum_recv.at[step, at],
            device_id=to(layer),
            device_id_type=pl.DeviceIdType.MESH,
        )

    def out_copy(at, step):
        i, layer, first, count = pieces[at]
        piece = new_w[i].at[layer, rows(i, behind(layer, step), first, count)]
        return pltpu.make_async_remote_copy(
            src_ref=piece,
            dst_ref=piece,
            send_sem=out_send.at[step, at],
            recv_sem=out_recv.at[step, at],
            device_id=to(layer),
            device_id_type=pl.DeviceIdType.MESH,
        )

    def landed(at, step):
        i, layer, first, count = pieces[at]
        return sums[i].at[layer, step, pl.ds(first, count)]

    def term(at, k):
        i, layer, first, count = pieces[at]
        return held[i].at[layer, rows(i, behind(layer, k), first, count)]

    def own_load(i, layer):
        return pltpu.make_async_copy(weights[i].at[layer, rows(i, me, 0, sums[i].shape[2])], own[i].at[layer], own_sem.at[i, layer])

    def moment_load(i):
        return (pltpu.make_async_copy(ms[i], new_m[i], m_sem.at[i]), pltpu.make_async_copy(vs[i], new_v[i], v_sem.at[i]))

    barrier = pltpu.get_barrier_semaphore()
    for neighbour in (left, right):
        pl.semaphore_signal(barrier, inc=1, device_id={AXIS: neighbour}, device_id_type=pl.DeviceIdType.MESH)
    pl.semaphore_wait(barrier, 2)

    for at, (i, layer, first, count) in enumerate(pieces):
        sum_copy(at, 0, terms[i].at[0, layer, rows(i, behind(layer, 1), first, count)]).start()

    for k in range(2, n + 1):
        for i, layer in every:
            load(i, layer, k).start()
    for i, layer in every:
        own_load(i, layer).start()
    for i in range(3):
        for copy in moment_load(i):
            copy.start()

    @pl.loop(0, n - 2)
    def _(step):
        for at, (i, layer, first, count) in enumerate(pieces):
            here = landed(at, step)
            sum_copy(at, step, here).wait_recv()
            if first == 0:
                load(i, layer, step + 2).wait()
            here[...] = (here[...].astype(jnp.float32) + term(at, step + 2)[...].astype(jnp.float32)).astype(jnp.bfloat16)
            sum_copy(at, step + 1, here).start()

    for i, layer in every:
        own_load(i, layer).wait()
    for i in range(3):
        for copy in moment_load(i):
            copy.wait()

    for at, (i, layer, first, count) in enumerate(pieces):
        here = landed(at, n - 2)
        sum_copy(at, n - 2, here).wait_recv()
        if first == 0:
            load(i, layer, n).wait()
        g = (here[...].astype(jnp.float32) + term(at, n)[...].astype(jnp.float32)).astype(jnp.bfloat16).astype(jnp.float32)
        piece = (layer, pl.ds(first, count))
        w, m, v = adamw(own[i][piece].astype(jnp.float32), new_m[i][piece], new_v[i][piece], g)
        new_w[i][layer, rows(i, me, first, count)] = w
        new_m[i][piece] = m
        new_v[i][piece] = v
        out_copy(at, 0).start()

    @pl.loop(0, n - 2)
    def _(step):
        for at in range(len(pieces)):
            out_copy(at, step).wait_recv()
            out_copy(at, step + 1).start()
        for at in range(len(pieces)):
            sum_copy(at, step, landed(at, step)).wait_send()

        @pl.when(step > 0)
        def _():
            for at in range(len(pieces)):
                out_copy(at, step - 1).wait_send()

    for at in range(len(pieces)):
        sum_copy(at, n - 2, landed(at, n - 2)).wait_send()
        out_copy(at, n - 3).wait_send()
    for at in range(len(pieces)):
        out_copy(at, n - 2).wait_recv()
    for at in range(len(pieces)):
        out_copy(at, n - 2).wait_send()


def put(*refs):
    count = len(refs) // 2
    halves = [(i, half) for i in range(count) for half in range(2)]
    copies = [
        pltpu.make_async_copy(
            refs[i].at[pl.ds(half * (refs[i].shape[0] // 2), refs[i].shape[0] // 2)],
            refs[count + i].at[pl.ds(half * (refs[i].shape[0] // 2), refs[i].shape[0] // 2)],
            refs[-1].at[i, half],
        )
        for i, half in halves
    ]
    for copy in copies:
        copy.start()
    for copy in copies:
        copy.wait()


def solution(mesh):
    n = mesh.shape[AXIS]

    def step(*arrays):
        terms, weights, m, v = (arrays[i : i + 3] for i in (0, 3, 6, 9))
        layers = m[0].shape[0]
        count = 3 * layers * PARTS
        dma = pltpu.SemaphoreType.DMA
        arrays = [pltpu.with_memory_space_constraint(one, pltpu.HBM) for one in arrays]
        new = pl.pallas_call(
            functools.partial(kernel, n),
            out_shape=tuple(pltpu.VMEM(w.shape, w.dtype) for w in weights) + tuple(pltpu.VMEM(one.shape, one.dtype) for one in m + v),
            in_specs=[pl.BlockSpec(memory_space=pltpu.HBM)] * 12,
            out_specs=(pl.BlockSpec(memory_space=pltpu.VMEM),) * 9,
            scratch_shapes=[pltpu.VMEM(w.shape, w.dtype) for w in weights]
            + [pltpu.VMEM((layers, n - 1, *one.shape[1:]), w.dtype) for w, one in zip(weights, m, strict=True)]
            + [pltpu.VMEM(one.shape, w.dtype) for w, one in zip(weights, m, strict=True)]
            + [dma((3, layers, n - 1)), dma((3, layers)), dma((3,)), dma((3,))]
            + [dma((n - 1, count))] * 4,
            compiler_params=pltpu.CompilerParams(collective_id=0, has_side_effects=True, vmem_limit_bytes=40 * 2**20),
        )(*arrays)
        new = [pltpu.with_memory_space_constraint(one, pltpu.VMEM) for one in new]
        return pl.pallas_call(
            put,
            out_shape=tuple(pltpu.HBM(one.shape, one.dtype) for one in new),
            in_specs=[pl.BlockSpec(memory_space=pltpu.VMEM)] * 9,
            out_specs=(pl.BlockSpec(memory_space=pltpu.HBM),) * 9,
            scratch_shapes=[dma((9, 2))],
            compiler_params=pltpu.CompilerParams(vmem_limit_bytes=2**20),
        )(*new)

    all_of, cut = P(None, None, None), P(None, AXIS, None)
    return jax.shard_map(
        step,
        mesh=mesh,
        in_specs=(P(("rep", AXIS), None, None, None),) * 3 + (all_of,) * 3 + (cut,) * 6,
        out_specs=(P("rep", None, None),) * 3 + (P("rep", AXIS, None),) * 6,
        check_vma=False,
    )
```

```python
import functools

import jax
import jax.numpy as jnp
from jax import lax
from jax.experimental import pallas as pl
from jax.experimental.pallas import tpu as pltpu
from jax.sharding import PartitionSpec as P

AXIS = "dp"
PARTS = 2


def adamw(w, m, v, g):
    m = 0.9 * m + 0.1 * g
    v = 0.95 * v + 0.05 * g * g
    step = m * lax.rsqrt(v + 1e-8) + 0.1 * w
    return (w - 0.02 * step).astype(jnp.bfloat16), m, v


def kernel(n, *refs):
    terms, weights, ms, vs = (refs[i : i + 3] for i in (0, 3, 6, 9))
    new_w, new_m, new_v = (refs[i : i + 3] for i in (12, 15, 18))
    held, sums, own = (refs[i : i + 3] for i in (21, 24, 27))
    first_sem, held_sem, own_sem, m_sem, v_sem, sum_send, sum_recv, out_send, out_recv = refs[30:]
    layers = held[0].shape[0]
    me = lax.axis_index(AXIS)
    right, left = lax.rem(me + 1, n), lax.rem(me + n - 1, n)
    every = [(i, layer) for i in range(3) for layer in range(layers)]
    pieces = [
        (i, layer, part * (sums[i].shape[2] // PARTS), sums[i].shape[2] // PARTS)
        for i in range(3)
        for part in range(PARTS)
        for half in range(layers // 2)
        for layer in (half, half + layers // 2)
    ]

    def rightward(layer):
        return layer < layers // 2

    def to(layer):
        return {AXIS: right if rightward(layer) else left}

    def behind(layer, k):
        return lax.rem(me + n - k if rightward(layer) else me + k, n)

    def rows(i, block, first, count):
        return pl.ds(pl.multiple_of(block * sums[i].shape[2] + first, 16), count)

    def load(i, layer, k):
        block = rows(i, behind(layer, k), 0, sums[i].shape[2])
        return pltpu.make_async_copy(terms[i].at[0, layer, block], held[i].at[layer, block], held_sem.at[i, layer, k - 2])

    def sum_copy(at, step, source):
        i, layer, first, count = pieces[at]
        return pltpu.make_async_remote_copy(
            src_ref=source,
            dst_ref=sums[i].at[layer, step, pl.ds(first, count)],
            send_sem=sum_send.at[step, at],
            recv_sem=sum_recv.at[step, at],
            device_id=to(layer),
            device_id_type=pl.DeviceIdType.MESH,
        )

    def out_copy(at, step):
        i, layer, first, count = pieces[at]
        piece = new_w[i].at[layer, rows(i, behind(layer, step), first, count)]
        return pltpu.make_async_remote_copy(
            src_ref=piece,
            dst_ref=piece,
            send_sem=out_send.at[step, at],
            recv_sem=out_recv.at[step, at],
            device_id=to(layer),
            device_id_type=pl.DeviceIdType.MESH,
        )

    def landed(at, step):
        i, layer, first, count = pieces[at]
        return sums[i].at[layer, step, pl.ds(first, count)]

    def term(at, k):
        i, layer, first, count = pieces[at]
        return held[i].at[layer, rows(i, behind(layer, k), first, count)]

    def first_load(at):
        i, layer, first, count = pieces[at]
        return pltpu.make_async_copy(terms[i].at[0, layer, rows(i, behind(layer, 1), first, count)], term(at, 1), first_sem.at[at])

    def own_load(i, layer):
        return pltpu.make_async_copy(weights[i].at[layer, rows(i, me, 0, sums[i].shape[2])], own[i].at[layer], own_sem.at[i, layer])

    def moment_load(i):
        return (pltpu.make_async_copy(ms[i], new_m[i], m_sem.at[i]), pltpu.make_async_copy(vs[i], new_v[i], v_sem.at[i]))

    barrier = pltpu.get_barrier_semaphore()
    for neighbour in (left, right):
        pl.semaphore_signal(barrier, inc=1, device_id={AXIS: neighbour}, device_id_type=pl.DeviceIdType.MESH)
    for at in range(len(pieces)):
        first_load(at).start()
    pl.semaphore_wait(barrier, 2)

    for at in range(len(pieces)):
        first_load(at).wait()
        sum_copy(at, 0, term(at, 1)).start()

    for k in range(2, n + 1):
        for i, layer in every:
            load(i, layer, k).start()
    for i, layer in every:
        own_load(i, layer).start()
    for i in range(3):
        for copy in moment_load(i):
            copy.start()

    @pl.loop(0, n - 2)
    def _(step):
        for at, (i, layer, first, count) in enumerate(pieces):
            here = landed(at, step)
            sum_copy(at, step, here).wait_recv()
            if first == 0:
                load(i, layer, step + 2).wait()
            here[...] = (here[...].astype(jnp.float32) + term(at, step + 2)[...].astype(jnp.float32)).astype(jnp.bfloat16)
            sum_copy(at, step + 1, here).start()

    for i, layer in every:
        own_load(i, layer).wait()
    for i in range(3):
        for copy in moment_load(i):
            copy.wait()

    for at, (i, layer, first, count) in enumerate(pieces):
        here = landed(at, n - 2)
        sum_copy(at, n - 2, here).wait_recv()
        if first == 0:
            load(i, layer, n).wait()
        g = (here[...].astype(jnp.float32) + term(at, n)[...].astype(jnp.float32)).astype(jnp.bfloat16).astype(jnp.float32)
        piece = (layer, pl.ds(first, count))
        w, m, v = adamw(own[i][piece].astype(jnp.float32), new_m[i][piece], new_v[i][piece], g)
        new_w[i][layer, rows(i, me, first, count)] = w
        new_m[i][piece] = m
        new_v[i][piece] = v
        out_copy(at, 0).start()

    @pl.loop(0, n - 2)
    def _(step):
        for at in range(len(pieces)):
            out_copy(at, step).wait_recv()
            out_copy(at, step + 1).start()
        for at in range(len(pieces)):
            sum_copy(at, step, landed(at, step)).wait_send()

        @pl.when(step > 0)
        def _():
            for at in range(len(pieces)):
                out_copy(at, step - 1).wait_send()

    for at in range(len(pieces)):
        sum_copy(at, n - 2, landed(at, n - 2)).wait_send()
        out_copy(at, n - 3).wait_send()
    for at in range(len(pieces)):
        out_copy(at, n - 2).wait_recv()
    for at in range(len(pieces)):
        out_copy(at, n - 2).wait_send()


def put(*refs):
    count = len(refs) // 2
    copies = [pltpu.make_async_copy(refs[i], refs[count + i], refs[-1].at[i]) for i in range(count)]
    for copy in copies:
        copy.start()
    for copy in copies:
        copy.wait()


def solution(mesh):
    n = mesh.shape[AXIS]

    def step(*arrays):
        terms, weights, m, v = (arrays[i : i + 3] for i in (0, 3, 6, 9))
        layers = m[0].shape[0]
        count = 3 * layers * PARTS
        dma = pltpu.SemaphoreType.DMA
        arrays = [pltpu.with_memory_space_constraint(one, pltpu.HBM) for one in arrays]
        new = pl.pallas_call(
            functools.partial(kernel, n),
            out_shape=tuple(pltpu.VMEM(w.shape, w.dtype) for w in weights) + tuple(pltpu.VMEM(one.shape, one.dtype) for one in m + v),
            in_specs=[pl.BlockSpec(memory_space=pltpu.HBM)] * 12,
            out_specs=(pl.BlockSpec(memory_space=pltpu.VMEM),) * 9,
            scratch_shapes=[pltpu.VMEM(w.shape, w.dtype) for w in weights]
            + [pltpu.VMEM((layers, n - 1, *one.shape[1:]), w.dtype) for w, one in zip(weights, m, strict=True)]
            + [pltpu.VMEM(one.shape, w.dtype) for w, one in zip(weights, m, strict=True)]
            + [dma((count,)), dma((3, layers, n - 1)), dma((3, layers)), dma((3,)), dma((3,))]
            + [dma((n - 1, count))] * 4,
            compiler_params=pltpu.CompilerParams(collective_id=0, has_side_effects=True, vmem_limit_bytes=40 * 2**20),
        )(*arrays)
        new = [pltpu.with_memory_space_constraint(one, pltpu.VMEM) for one in new]
        return pl.pallas_call(
            put,
            out_shape=tuple(pltpu.HBM(one.shape, one.dtype) for one in new),
            in_specs=[pl.BlockSpec(memory_space=pltpu.VMEM)] * 9,
            out_specs=(pl.BlockSpec(memory_space=pltpu.HBM),) * 9,
            scratch_shapes=[dma((9,))],
            compiler_params=pltpu.CompilerParams(vmem_limit_bytes=2**20),
        )(*new)

    all_of, cut = P(None, None, None), P(None, AXIS, None)
    return jax.shard_map(
        step,
        mesh=mesh,
        in_specs=(P(("rep", AXIS), None, None, None),) * 3 + (all_of,) * 3 + (cut,) * 6,
        out_specs=(P("rep", None, None),) * 3 + (P("rep", AXIS, None),) * 6,
        check_vma=False,
    )
```

```python
import functools

import jax
import jax.numpy as jnp
from jax import lax
from jax.experimental import pallas as pl
from jax.experimental.pallas import tpu as pltpu
from jax.sharding import PartitionSpec as P

AXIS = "dp"
PARTS = 1


def adamw(w, m, v, g):
    m = 0.9 * m + 0.1 * g
    v = 0.95 * v + 0.05 * g * g
    step = m * lax.rsqrt(v + 1e-8) + 0.1 * w
    return (w - 0.02 * step).astype(jnp.bfloat16), m, v


def cut(rows):
    edges = [16 * (rows // 16 * part // PARTS) for part in range(PARTS)] + [rows]
    return [(a, b - a) for a, b in zip(edges, edges[1:])]


def kernel(n, *refs):
    terms, weights, ms, vs = (refs[i : i + 3] for i in (0, 3, 6, 9))
    new_w, new_m, new_v = (refs[i : i + 3] for i in (12, 15, 18))
    held, sums, own = (refs[i : i + 3] for i in (21, 24, 27))
    held_sem, own_sem, m_sem, v_sem, sum_send, sum_recv, out_send, out_recv = refs[30:]
    layers = held[0].shape[0]
    me = lax.axis_index(AXIS)
    right, left = lax.rem(me + 1, n), lax.rem(me + n - 1, n)
    every = [(i, layer) for i in range(3) for layer in range(layers)]
    pieces = [
        (i, layer, *cut(sums[i].shape[2])[part])
        for i in range(3)
        for part in range(PARTS)
        for half in range(layers // 2)
        for layer in (half, half + layers // 2)
    ]

    def rightward(layer):
        return layer < layers // 2

    def to(layer):
        return {AXIS: right if rightward(layer) else left}

    def behind(layer, k):
        return lax.rem(me + n - k if rightward(layer) else me + k, n)

    def rows(i, block, first, count):
        return pl.ds(pl.multiple_of(block * sums[i].shape[2] + first, 16), count)

    def load(i, layer, k):
        block = rows(i, behind(layer, k), 0, sums[i].shape[2])
        return pltpu.make_async_copy(terms[i].at[0, layer, block], held[i].at[layer, block], held_sem.at[i, layer, k - 2])

    def sum_copy(at, step, source):
        i, layer, first, count = pieces[at]
        return pltpu.make_async_remote_copy(
            src_ref=source,
            dst_ref=sums[i].at[layer, step, pl.ds(first, count)],
            send_sem=sum_send.at[step, at],
            recv_sem=sum_recv.at[step, at],
            device_id=to(layer),
            device_id_type=pl.DeviceIdType.MESH,
        )

    def out_copy(at, step):
        i, layer, first, count = pieces[at]
        piece = new_w[i].at[layer, rows(i, behind(layer, step), first, count)]
        return pltpu.make_async_remote_copy(
            src_ref=piece,
            dst_ref=piece,
            send_sem=out_send.at[step, at],
            recv_sem=out_recv.at[step, at],
            device_id=to(layer),
            device_id_type=pl.DeviceIdType.MESH,
        )

    def landed(at, step):
        i, layer, first, count = pieces[at]
        return sums[i].at[layer, step, pl.ds(first, count)]

    def term(at, k):
        i, layer, first, count = pieces[at]
        return held[i].at[layer, rows(i, behind(layer, k), first, count)]

    def own_load(i, layer):
        return pltpu.make_async_copy(weights[i].at[layer, rows(i, me, 0, sums[i].shape[2])], own[i].at[layer], own_sem.at[i, layer])

    def moment_load(i):
        return (pltpu.make_async_copy(ms[i], new_m[i], m_sem.at[i]), pltpu.make_async_copy(vs[i], new_v[i], v_sem.at[i]))

    barrier = pltpu.get_barrier_semaphore()
    for neighbour in (left, right):
        pl.semaphore_signal(barrier, inc=1, device_id={AXIS: neighbour}, device_id_type=pl.DeviceIdType.MESH)
    pl.semaphore_wait(barrier, 2)

    for at, (i, layer, first, count) in enumerate(pieces):
        sum_copy(at, 0, terms[i].at[0, layer, rows(i, behind(layer, 1), first, count)]).start()

    for k in range(2, n + 1):
        for i, layer in every:
            load(i, layer, k).start()
    for i, layer in every:
        own_load(i, layer).start()
    for i in range(3):
        for copy in moment_load(i):
            copy.start()

    @pl.loop(0, n - 2)
    def _(step):
        for at, (i, layer, first, count) in enumerate(pieces):
            here = landed(at, step)
            sum_copy(at, step, here).wait_recv()
            if first == 0:
                load(i, layer, step + 2).wait()
            here[...] = (here[...].astype(jnp.float32) + term(at, step + 2)[...].astype(jnp.float32)).astype(jnp.bfloat16)
            sum_copy(at, step + 1, here).start()

    for i, layer in every:
        own_load(i, layer).wait()
    for i in range(3):
        for copy in moment_load(i):
            copy.wait()

    for at, (i, layer, first, count) in enumerate(pieces):
        here = landed(at, n - 2)
        sum_copy(at, n - 2, here).wait_recv()
        if first == 0:
            load(i, layer, n).wait()
        g = (here[...].astype(jnp.float32) + term(at, n)[...].astype(jnp.float32)).astype(jnp.bfloat16).astype(jnp.float32)
        piece = (layer, pl.ds(first, count))
        w, m, v = adamw(own[i][piece].astype(jnp.float32), new_m[i][piece], new_v[i][piece], g)
        new_w[i][layer, rows(i, me, first, count)] = w
        new_m[i][piece] = m
        new_v[i][piece] = v
        out_copy(at, 0).start()

    @pl.loop(0, n - 2)
    def _(step):
        for at in range(len(pieces)):
            out_copy(at, step).wait_recv()
            out_copy(at, step + 1).start()
        for at in range(len(pieces)):
            sum_copy(at, step, landed(at, step)).wait_send()

        @pl.when(step > 0)
        def _():
            for at in range(len(pieces)):
                out_copy(at, step - 1).wait_send()

    for at in range(len(pieces)):
        sum_copy(at, n - 2, landed(at, n - 2)).wait_send()
        out_copy(at, n - 3).wait_send()
    for at in range(len(pieces)):
        out_copy(at, n - 2).wait_recv()
    for at in range(len(pieces)):
        out_copy(at, n - 2).wait_send()


def put(*refs):
    count = len(refs) // 2
    copies = [pltpu.make_async_copy(refs[i], refs[count + i], refs[-1].at[i]) for i in range(count)]
    for copy in copies:
        copy.start()
    for copy in copies:
        copy.wait()


def solution(mesh):
    n = mesh.shape[AXIS]

    def step(*arrays):
        terms, weights, m, v = (arrays[i : i + 3] for i in (0, 3, 6, 9))
        layers = m[0].shape[0]
        count = 3 * layers * PARTS
        dma = pltpu.SemaphoreType.DMA
        arrays = [pltpu.with_memory_space_constraint(one, pltpu.HBM) for one in arrays]
        new = pl.pallas_call(
            functools.partial(kernel, n),
            out_shape=tuple(pltpu.VMEM(w.shape, w.dtype) for w in weights) + tuple(pltpu.VMEM(one.shape, one.dtype) for one in m + v),
            in_specs=[pl.BlockSpec(memory_space=pltpu.HBM)] * 12,
            out_specs=(pl.BlockSpec(memory_space=pltpu.VMEM),) * 9,
            scratch_shapes=[pltpu.VMEM(w.shape, w.dtype) for w in weights]
            + [pltpu.VMEM((layers, n - 1, *one.shape[1:]), w.dtype) for w, one in zip(weights, m, strict=True)]
            + [pltpu.VMEM(one.shape, w.dtype) for w, one in zip(weights, m, strict=True)]
            + [dma((3, layers, n - 1)), dma((3, layers)), dma((3,)), dma((3,))]
            + [dma((n - 1, count))] * 4,
            compiler_params=pltpu.CompilerParams(collective_id=0, has_side_effects=True, vmem_limit_bytes=40 * 2**20),
        )(*arrays)
        new = [pltpu.with_memory_space_constraint(one, pltpu.VMEM) for one in new]
        return pl.pallas_call(
            put,
            out_shape=tuple(pltpu.HBM(one.shape, one.dtype) for one in new),
            in_specs=[pl.BlockSpec(memory_space=pltpu.VMEM)] * 9,
            out_specs=(pl.BlockSpec(memory_space=pltpu.HBM),) * 9,
            scratch_shapes=[dma((9,))],
            compiler_params=pltpu.CompilerParams(vmem_limit_bytes=2**20),
        )(*new)

    all_of, part = P(None, None, None), P(None, AXIS, None)
    return jax.shard_map(
        step,
        mesh=mesh,
        in_specs=(P(("rep", AXIS), None, None, None),) * 3 + (all_of,) * 3 + (part,) * 6,
        out_specs=(P("rep", None, None),) * 3 + (P("rep", AXIS, None),) * 6,
        check_vma=False,
    )
```

```python
import functools

import jax
import jax.numpy as jnp
from jax import lax
from jax.experimental import pallas as pl
from jax.experimental.pallas import tpu as pltpu
from jax.sharding import PartitionSpec as P

AXIS = "dp"
PARTS = 1


def adamw(w, m, v, g):
    m = 0.9 * m + 0.1 * g
    v = 0.95 * v + 0.05 * g * g
    step = m * lax.rsqrt(v + 1e-8) + 0.1 * w
    return (w - 0.02 * step).astype(jnp.bfloat16), m, v


def cut(rows):
    edges = [16 * (rows // 16 * part // PARTS) for part in range(PARTS)] + [rows]
    return [(a, b - a) for a, b in zip(edges, edges[1:])]


def kernel(n, *refs):
    terms, weights, ms, vs = (refs[i : i + 3] for i in (0, 3, 6, 9))
    new_w, new_m, new_v = (refs[i : i + 3] for i in (12, 15, 18))
    held, sums, own = (refs[i : i + 3] for i in (21, 24, 27))
    entered, held_sem, own_sem, m_sem, v_sem, sum_send, sum_recv, out_send, out_recv = refs[30:]
    layers = held[0].shape[0]
    me = lax.axis_index(AXIS)
    right, left = lax.rem(me + 1, n), lax.rem(me + n - 1, n)
    every = [(i, layer) for i in range(3) for layer in range(layers)]
    pieces = [
        (i, layer, *cut(sums[i].shape[2])[part])
        for i in range(3)
        for part in range(PARTS)
        for half in range(layers // 2)
        for layer in (half, half + layers // 2)
    ]

    def rightward(layer):
        return layer < layers // 2

    def to(layer):
        return {AXIS: right if rightward(layer) else left}

    def behind(layer, k):
        return lax.rem(me + n - k if rightward(layer) else me + k, n)

    def rows(i, block, first, count):
        return pl.ds(pl.multiple_of(block * sums[i].shape[2] + first, 16), count)

    def load(i, layer, k):
        block = rows(i, behind(layer, k), 0, sums[i].shape[2])
        return pltpu.make_async_copy(terms[i].at[0, layer, block], held[i].at[layer, block], held_sem.at[i, layer, k - 2])

    def sum_copy(at, step, source):
        i, layer, first, count = pieces[at]
        return pltpu.make_async_remote_copy(
            src_ref=source,
            dst_ref=sums[i].at[layer, step, pl.ds(first, count)],
            send_sem=sum_send.at[step, at],
            recv_sem=sum_recv.at[step, at],
            device_id=to(layer),
            device_id_type=pl.DeviceIdType.MESH,
        )

    def out_copy(at, step):
        i, layer, first, count = pieces[at]
        piece = new_w[i].at[layer, rows(i, behind(layer, step), first, count)]
        return pltpu.make_async_remote_copy(
            src_ref=piece,
            dst_ref=piece,
            send_sem=out_send.at[step, at],
            recv_sem=out_recv.at[step, at],
            device_id=to(layer),
            device_id_type=pl.DeviceIdType.MESH,
        )

    def landed(at, step):
        i, layer, first, count = pieces[at]
        return sums[i].at[layer, step, pl.ds(first, count)]

    def term(at, k):
        i, layer, first, count = pieces[at]
        return held[i].at[layer, rows(i, behind(layer, k), first, count)]

    def own_load(i, layer):
        return pltpu.make_async_copy(weights[i].at[layer, rows(i, me, 0, sums[i].shape[2])], own[i].at[layer], own_sem.at[i, layer])

    def moment_load(i):
        return (pltpu.make_async_copy(ms[i], new_m[i], m_sem.at[i]), pltpu.make_async_copy(vs[i], new_v[i], v_sem.at[i]))

    barrier = pltpu.get_barrier_semaphore()
    pl.semaphore_signal(barrier, inc=1, device_id={AXIS: left}, device_id_type=pl.DeviceIdType.MESH)
    pl.semaphore_wait(barrier, 1)
    pl.semaphore_signal(entered, inc=1, device_id={AXIS: right}, device_id_type=pl.DeviceIdType.MESH)
    for rightbound in (True, False):
        if not rightbound:
            pl.semaphore_wait(entered, 1)
        for at, (i, layer, first, count) in enumerate(pieces):
            if rightward(layer) == rightbound:
                sum_copy(at, 0, terms[i].at[0, layer, rows(i, behind(layer, 1), first, count)]).start()

    for k in range(2, n + 1):
        for i, layer in every:
            load(i, layer, k).start()
    for i, layer in every:
        own_load(i, layer).start()
    for i in range(3):
        for copy in moment_load(i):
            copy.start()

    @pl.loop(0, n - 2)
    def _(step):
        for at, (i, layer, first, count) in enumerate(pieces):
            here = landed(at, step)
            sum_copy(at, step, here).wait_recv()
            if first == 0:
                load(i, layer, step + 2).wait()
            here[...] = (here[...].astype(jnp.float32) + term(at, step + 2)[...].astype(jnp.float32)).astype(jnp.bfloat16)
            sum_copy(at, step + 1, here).start()

    for i, layer in every:
        own_load(i, layer).wait()
    for i in range(3):
        for copy in moment_load(i):
            copy.wait()

    for at, (i, layer, first, count) in enumerate(pieces):
        here = landed(at, n - 2)
        sum_copy(at, n - 2, here).wait_recv()
        if first == 0:
            load(i, layer, n).wait()
        g = (here[...].astype(jnp.float32) + term(at, n)[...].astype(jnp.float32)).astype(jnp.bfloat16).astype(jnp.float32)
        piece = (layer, pl.ds(first, count))
        w, m, v = adamw(own[i][piece].astype(jnp.float32), new_m[i][piece], new_v[i][piece], g)
        new_w[i][layer, rows(i, me, first, count)] = w
        new_m[i][piece] = m
        new_v[i][piece] = v
        out_copy(at, 0).start()

    @pl.loop(0, n - 2)
    def _(step):
        for at in range(len(pieces)):
            out_copy(at, step).wait_recv()
            out_copy(at, step + 1).start()
        for at in range(len(pieces)):
            sum_copy(at, step, landed(at, step)).wait_send()

        @pl.when(step > 0)
        def _():
            for at in range(len(pieces)):
                out_copy(at, step - 1).wait_send()

    for at in range(len(pieces)):
        sum_copy(at, n - 2, landed(at, n - 2)).wait_send()
        out_copy(at, n - 3).wait_send()
    for at in range(len(pieces)):
        out_copy(at, n - 2).wait_recv()
    for at in range(len(pieces)):
        out_copy(at, n - 2).wait_send()


def put(*refs):
    count = len(refs) // 2
    copies = [pltpu.make_async_copy(refs[i], refs[count + i], refs[-1].at[i]) for i in range(count)]
    for copy in copies:
        copy.start()
    for copy in copies:
        copy.wait()


def solution(mesh):
    n = mesh.shape[AXIS]

    def step(*arrays):
        terms, weights, m, v = (arrays[i : i + 3] for i in (0, 3, 6, 9))
        layers = m[0].shape[0]
        count = 3 * layers * PARTS
        dma = pltpu.SemaphoreType.DMA
        arrays = [pltpu.with_memory_space_constraint(one, pltpu.HBM) for one in arrays]
        new = pl.pallas_call(
            functools.partial(kernel, n),
            out_shape=tuple(pltpu.VMEM(w.shape, w.dtype) for w in weights) + tuple(pltpu.VMEM(one.shape, one.dtype) for one in m + v),
            in_specs=[pl.BlockSpec(memory_space=pltpu.HBM)] * 12,
            out_specs=(pl.BlockSpec(memory_space=pltpu.VMEM),) * 9,
            scratch_shapes=[pltpu.VMEM(w.shape, w.dtype) for w in weights]
            + [pltpu.VMEM((layers, n - 1, *one.shape[1:]), w.dtype) for w, one in zip(weights, m, strict=True)]
            + [pltpu.VMEM(one.shape, w.dtype) for w, one in zip(weights, m, strict=True)]
            + [pltpu.SemaphoreType.REGULAR, dma((3, layers, n - 1)), dma((3, layers)), dma((3,)), dma((3,))]
            + [dma((n - 1, count))] * 4,
            compiler_params=pltpu.CompilerParams(collective_id=0, has_side_effects=True, vmem_limit_bytes=40 * 2**20),
        )(*arrays)
        new = [pltpu.with_memory_space_constraint(one, pltpu.VMEM) for one in new]
        return pl.pallas_call(
            put,
            out_shape=tuple(pltpu.HBM(one.shape, one.dtype) for one in new),
            in_specs=[pl.BlockSpec(memory_space=pltpu.VMEM)] * 9,
            out_specs=(pl.BlockSpec(memory_space=pltpu.HBM),) * 9,
            scratch_shapes=[dma((9,))],
            compiler_params=pltpu.CompilerParams(vmem_limit_bytes=2**20),
        )(*new)

    all_of, part = P(None, None, None), P(None, AXIS, None)
    return jax.shard_map(
        step,
        mesh=mesh,
        in_specs=(P(("rep", AXIS), None, None, None),) * 3 + (all_of,) * 3 + (part,) * 6,
        out_specs=(P("rep", None, None),) * 3 + (P("rep", AXIS, None),) * 6,
        check_vma=False,
    )
```

```python
import functools

import jax
import jax.numpy as jnp
from jax import lax
from jax.experimental import pallas as pl
from jax.experimental.pallas import tpu as pltpu
from jax.sharding import PartitionSpec as P

AXIS = "dp"
MESH = pl.DeviceIdType.MESH


def adamw(w, m, v, g):
    m = 0.9 * m + 0.1 * g
    v = 0.95 * v + 0.05 * g * g
    step = m * lax.rsqrt(v + 1e-8) + 0.1 * w
    return (w - 0.02 * step).astype(jnp.bfloat16), m, v


def stacks_of(moments):
    by_shape = {}
    for i, one in enumerate(moments):
        by_shape.setdefault(one.shape, []).append(i)
    return list(by_shape.values())


def kernel(n, stacks, *refs):
    terms, weights, ms, vs = (refs[i : i + 3] for i in (0, 3, 6, 9))
    k = len(stacks)
    new_w, new_m, new_v = refs[12 : 12 + k], refs[12 + k : 15 + k], refs[15 + k : 18 + k]
    held, own, sums = refs[18 + k : 21 + k], refs[21 + k : 24 + k], refs[24 + k : 24 + 2 * k]
    entered, held_sem, own_sem, m_sem, v_sem, first_send, first_recv, sum_send, sum_recv, out_send, out_recv = refs[24 + 2 * k :]
    layers, block = own[0].shape[0], [one.shape[1] for one in own]
    me = lax.axis_index(AXIS)
    right, left = lax.rem(me + 1, n), lax.rem(me + n - 1, n)
    turns = [layer for half in range(layers // 2) for layer in (half, half + layers // 2)]
    every = [(i, layer) for stack in stacks for layer in turns for i in stack]
    loads = [(s, layer) for s in range(k) for layer in turns]

    def rightward(layer):
        return layer < layers // 2

    def behind(layer, steps):
        return lax.rem(me + n - steps if rightward(layer) else me + steps, n)

    def rows(i, device):
        return pl.ds(pl.multiple_of(device * block[i], 16), block[i])

    def send(layer, source, target, send_sem, recv_sem):
        return pltpu.make_async_remote_copy(
            src_ref=source,
            dst_ref=target,
            send_sem=send_sem,
            recv_sem=recv_sem,
            device_id={AXIS: right if rightward(layer) else left},
            device_id_type=MESH,
        )

    def first_copy(i, layer):
        s, place = next((s, stack.index(i)) for s, stack in enumerate(stacks) if i in stack)
        source = terms[i].at[0, layer, rows(i, behind(layer, 1))]
        return send(layer, source, sums[s].at[layer, 0, place], first_send.at[i, layer], first_recv.at[i, layer])

    def sum_copy(s, layer, step):
        return send(layer, sums[s].at[layer, step - 1], sums[s].at[layer, step], sum_send.at[step - 1, s, layer], sum_recv.at[step - 1, s, layer])

    def out_copy(s, layer, step):
        piece = new_w[s].at[layer, behind(layer, step)]
        return send(layer, piece, piece, out_send.at[step, s, layer], out_recv.at[step, s, layer])

    def load(i, layer, steps):
        part = rows(i, behind(layer, steps))
        return pltpu.make_async_copy(terms[i].at[0, layer, part], held[i].at[layer, part], held_sem.at[i, layer, steps - 2])

    def own_load(i):
        return pltpu.make_async_copy(weights[i].at[:, rows(i, me)], own[i], own_sem.at[i])

    def moment_load(i):
        return (pltpu.make_async_copy(ms[i], new_m[i], m_sem.at[i]), pltpu.make_async_copy(vs[i], new_v[i], v_sem.at[i]))

    def total(s, layer, step, place):
        i = stacks[s][place]
        load(i, layer, step + 2).wait()
        term = held[i][layer, rows(i, behind(layer, step + 2)), :]
        return (sums[s][layer, step, place].astype(jnp.float32) + term.astype(jnp.float32)).astype(jnp.bfloat16)

    barrier = pltpu.get_barrier_semaphore()
    pl.semaphore_signal(barrier, inc=1, device_id={AXIS: left}, device_id_type=MESH)
    pl.semaphore_wait(barrier, 1)
    pl.semaphore_signal(entered, inc=1, device_id={AXIS: right}, device_id_type=MESH)
    for i, layer in every:
        if rightward(layer):
            first_copy(i, layer).start()
    pl.semaphore_wait(entered, 1)
    for i, layer in every:
        if not rightward(layer):
            first_copy(i, layer).start()

    for steps in range(2, n + 1):
        for i, layer in every:
            load(i, layer, steps).start()
    for i in range(3):
        own_load(i).start()
        for copy in moment_load(i):
            copy.start()

    def add_and_send(s, layer, step):
        for place in range(len(stacks[s])):
            sums[s][layer, step, place] = total(s, layer, step, place)
        sum_copy(s, layer, step + 1).start()

    for s, layer in loads:
        for i in stacks[s]:
            first_copy(i, layer).wait_recv()
        add_and_send(s, layer, 0)

    @pl.loop(1, n - 2)
    def _(step):
        for s, layer in loads:
            sum_copy(s, layer, step).wait_recv()
            add_and_send(s, layer, step)

    for i in range(3):
        own_load(i).wait()
        for copy in moment_load(i):
            copy.wait()

    for s, layer in loads:
        sum_copy(s, layer, n - 2).wait_recv()
        for place, i in enumerate(stacks[s]):
            g = total(s, layer, n - 2, place).astype(jnp.float32)
            w, m, v = adamw(own[i][layer].astype(jnp.float32), new_m[i][layer], new_v[i][layer], g)
            new_w[s][layer, me, place] = w
            new_m[i][layer] = m
            new_v[i][layer] = v
        out_copy(s, layer, 0).start()

    for i, layer in every:
        first_copy(i, layer).wait_send()

    @pl.loop(0, n - 2)
    def _(step):
        for s, layer in loads:
            out_copy(s, layer, step).wait_recv()
            out_copy(s, layer, step + 1).start()
        for s, layer in loads:
            sum_copy(s, layer, step + 1).wait_send()

        @pl.when(step > 0)
        def _():
            for s, layer in loads:
                out_copy(s, layer, step - 1).wait_send()

    for s, layer in loads:
        out_copy(s, layer, n - 3).wait_send()
    for s, layer in loads:
        out_copy(s, layer, n - 2).wait_recv()
    for s, layer in loads:
        out_copy(s, layer, n - 2).wait_send()


def put(stacks, *refs):
    stacked, moments = refs[: len(stacks)], refs[len(stacks) : len(stacks) + 6]
    outs, sem = refs[len(stacks) + 6 : -1], refs[-1]
    sources = list(moments)
    for i in reversed(range(3)):
        s, place = next((s, stack.index(i)) for s, stack in enumerate(stacks) if i in stack)
        sources.insert(0, stacked[s].at[:, :, place])
    copies = [pltpu.make_async_copy(source, out, sem.at[i]) for i, (source, out) in enumerate(zip(sources, outs, strict=True))]
    for copy in copies:
        copy.start()
    for copy in copies:
        copy.wait()


def solution(mesh):
    n = mesh.shape[AXIS]

    def step(*arrays):
        terms, weights, m, v = (arrays[i : i + 3] for i in (0, 3, 6, 9))
        layers = m[0].shape[0]
        stacks = stacks_of(m)
        dma = pltpu.SemaphoreType.DMA
        stack_shapes = [(len(stack), *m[stack[0]].shape[1:]) for stack in stacks]
        arrays = [pltpu.with_memory_space_constraint(one, pltpu.HBM) for one in arrays]
        new = pl.pallas_call(
            functools.partial(kernel, n, stacks),
            out_shape=tuple(pltpu.VMEM((layers, n, *shape), weights[0].dtype) for shape in stack_shapes)
            + tuple(pltpu.VMEM(one.shape, one.dtype) for one in m + v),
            in_specs=[pl.BlockSpec(memory_space=pltpu.HBM)] * 12,
            out_specs=(pl.BlockSpec(memory_space=pltpu.VMEM),) * (6 + len(stacks)),
            scratch_shapes=[pltpu.VMEM(w.shape, w.dtype) for w in weights]
            + [pltpu.VMEM(one.shape, w.dtype) for w, one in zip(weights, m, strict=True)]
            + [pltpu.VMEM((layers, n - 1, *shape), weights[0].dtype) for shape in stack_shapes]
            + [pltpu.SemaphoreType.REGULAR, dma((3, layers, n - 1)), dma((3,)), dma((3,)), dma((3,))]
            + [dma((3, layers))] * 2
            + [dma((n - 2, len(stacks), layers))] * 2
            + [dma((n - 1, len(stacks), layers))] * 2,
            compiler_params=pltpu.CompilerParams(collective_id=0, has_side_effects=True, vmem_limit_bytes=40 * 2**20),
        )(*arrays)
        new = [pltpu.with_memory_space_constraint(one, pltpu.VMEM) for one in new]
        outs = pl.pallas_call(
            functools.partial(put, stacks),
            out_shape=tuple(pltpu.HBM((layers, n, *one.shape[1:]), w.dtype) for w, one in zip(weights, m, strict=True))
            + tuple(pltpu.HBM(one.shape, one.dtype) for one in m + v),
            in_specs=[pl.BlockSpec(memory_space=pltpu.VMEM)] * (6 + len(stacks)),
            out_specs=(pl.BlockSpec(memory_space=pltpu.HBM),) * 9,
            scratch_shapes=[dma((9,))],
            compiler_params=pltpu.CompilerParams(vmem_limit_bytes=2**20),
        )(*new)
        return (*(out.reshape(w.shape) for out, w in zip(outs[:3], weights, strict=True)), *outs[3:])

    all_of, part = P(None, None, None), P(None, AXIS, None)
    return jax.shard_map(
        step,
        mesh=mesh,
        in_specs=(P(("rep", AXIS), None, None, None),) * 3 + (all_of,) * 3 + (part,) * 6,
        out_specs=(P("rep", None, None),) * 3 + (P("rep", AXIS, None),) * 6,
        check_vma=False,
    )
```

```python
import functools

import jax
import jax.numpy as jnp
from jax import lax
from jax.experimental import pallas as pl
from jax.experimental.pallas import tpu as pltpu
from jax.sharding import PartitionSpec as P

AXIS = "dp"
MESH = pl.DeviceIdType.MESH
ROWS, LANES = 16, 128
MOVED = 1


def adamw(w, m, v, g):
    m = 0.9 * m + 0.1 * g
    v = 0.95 * v + 0.05 * g * g
    step = m * lax.rsqrt(v + 1e-8) + 0.1 * w
    return (w - 0.02 * step).astype(jnp.bfloat16), m, v


class Plan:
    def __init__(self, shapes):
        self.layers = shapes[0][0]
        self.block = [shape[1] for shape in shapes]
        self.wide = [shape[2] // LANES for shape in shapes]
        half = self.layers // 2
        order = sorted(range(len(shapes)), key=lambda i: (self.wide[i], i))
        bands, tile = {}, 0
        for rightward in (False, True):
            bands[rightward] = []
            for layer in range(half) if rightward else range(half, self.layers):
                for i in order:
                    for row in range(self.block[i] // ROWS):
                        bands[rightward].append((layer, i, row, tile))
                        tile += self.wide[i]
        self.tiles = tile
        self.sums = self.cut(bands[False], bands[True])
        self.news = self.cut(bands[False] + bands[True][:MOVED], bands[True][MOVED:])

    def cut(self, left, right):
        copies = []
        for rightward, bands in ((True, right), (False, left)):
            count = sum(self.wide[i] for _, i, _, _ in bands)
            at = next(k for k, band in enumerate(bands) if 2 * (band[3] - bands[0][3]) >= count - self.wide[band[1]])
            copies.append([(rightward, part) for part in (bands[:at], bands[at:])])
        return [
            (rightward, part[0][3], sum(self.wide[i] for _, i, _, _ in part), self.runs(part))
            for pair in zip(*copies)
            for rightward, part in pair
        ]

    def runs(self, bands):
        runs = []
        for layer, i, row, tile in bands:
            if runs and runs[-1][:2] == [layer, i]:
                runs[-1][3] += 1
            else:
                runs.append([layer, i, row, 1, tile])
        return runs


def kernel(n, plan, *refs):
    terms, weights, ms, vs = (refs[i : i + 3] for i in (0, 3, 6, 9))
    new_w, new_m, new_v, held, own, first = (refs[i : i + 3] for i in (12, 15, 18, 21, 24, 27))
    sums, news, entered, held_sem, own_sem, m_sem, v_sem, first_send, first_recv, sum_send, sum_recv, out_send, out_recv = refs[30:]
    me = lax.axis_index(AXIS)
    right, left = lax.rem(me + 1, n), lax.rem(me + n - 1, n)
    half = plan.layers // 2
    every = [(i, layer) for i in sorted(range(3), key=lambda i: (plan.wide[i], i)) for pair in range(half) for layer in (pair, half + pair)]

    def behind(rightward, steps):
        return lax.rem(me + n - steps if rightward else me + steps, n)

    def rows(i, device):
        return pl.ds(pl.multiple_of(device * plan.block[i], ROWS), plan.block[i])

    def send(rightward, source, target, send_sem, recv_sem):
        return pltpu.make_async_remote_copy(
            src_ref=source,
            dst_ref=target,
            send_sem=send_sem,
            recv_sem=recv_sem,
            device_id={AXIS: right if rightward else left},
            device_id_type=MESH,
        )

    def first_copy(i, layer):
        rightward = layer < half
        source = terms[i].at[0, layer, rows(i, behind(rightward, 1))]
        return send(rightward, source, first[i].at[layer], first_send.at[i, layer], first_recv.at[i, layer])

    def sum_copy(at, step):
        rightward, tile, count, _ = plan.sums[at]
        part = pl.ds(tile, count)
        return send(rightward, sums.at[step - 1, part], sums.at[step, part], sum_send.at[step - 1, at], sum_recv.at[step - 1, at])

    def out_copy(at, step):
        rightward, tile, count, _ = plan.news[at]
        piece = news.at[behind(rightward, step), pl.ds(tile, count)]
        return send(rightward, piece, piece, out_send.at[step, at], out_recv.at[step, at])

    def load(i, layer, steps):
        part = rows(i, behind(layer < half, steps))
        return pltpu.make_async_copy(terms[i].at[0, layer, part], held[i].at[layer, part], held_sem.at[i, layer, steps - 2])

    def own_load(i):
        return pltpu.make_async_copy(weights[i].at[:, rows(i, me)], own[i], own_sem.at[i])

    def moment_load(i):
        return (pltpu.make_async_copy(ms[i], new_m[i], m_sem.at[i]), pltpu.make_async_copy(vs[i], new_v[i], v_sem.at[i]))

    def each_tile(runs, body):
        for layer, i, row, count, tile in runs:

            @pl.loop(0, count)
            def _(k, layer=layer, i=i, row=row, tile=tile):
                for column in range(plan.wide[i]):
                    body(layer, i, (row + k) * ROWS, column * LANES, tile + k * plan.wide[i] + column)

    def tile_of(ref, layer, row, column):
        return ref[layer, pl.ds(pl.multiple_of(row, ROWS), ROWS), pl.ds(column, LANES)]

    def term(i, layer, steps, row, column):
        device = behind(layer < half, steps)
        return tile_of(held[i], layer, device * plan.block[i] + row, column).astype(jnp.float32)

    barrier = pltpu.get_barrier_semaphore()

    @pl.when(me < n - 1)
    def _():
        pl.semaphore_signal(barrier, inc=1, device_id={AXIS: right}, device_id_type=MESH)

    @pl.when(me == 0)
    def _():
        pl.semaphore_signal(barrier, inc=1, device_id={AXIS: left}, device_id_type=MESH)

    def start(rightward):
        for i, layer in every:
            if (layer < half) == rightward:
                first_copy(i, layer).start()


    @pl.when(me > 0)
    def _():
        pl.semaphore_wait(barrier, 1 + (me == n - 1).astype(jnp.int32))
        pl.semaphore_signal(entered.at[1], inc=1, device_id={AXIS: left}, device_id_type=MESH)

    @pl.when(me == n - 1)
    def _():
        pl.semaphore_signal(entered.at[0], inc=1, device_id={AXIS: right}, device_id_type=MESH)
        start(True)

    @pl.when(me > 0)
    def _():
        start(False)

    @pl.when(me < n - 1)
    def _():
        pl.semaphore_wait(entered.at[1], 1)
        start(True)

    @pl.when(me == 0)
    def _():
        pl.semaphore_wait(entered.at[0], 1)
        start(False)

    for steps in range(2, n + 1):
        for i, layer in every:
            load(i, layer, steps).start()
    for i in range(3):
        own_load(i).start()
        for copy in moment_load(i):
            copy.start()

    def wait_loads(runs, steps):
        for layer, i, row, _, _ in runs:
            if row == 0:
                load(i, layer, steps).wait()

    arrived = set()
    for at, (rightward, _, _, runs) in enumerate(plan.sums):
        for layer, i, row, _, _ in runs:
            if (i, layer) not in arrived:
                first_copy(i, layer).wait_recv()
                arrived.add((i, layer))
        wait_loads(runs, 2)

        def add_first(layer, i, row, column, tile):
            sums[0, tile] = (tile_of(first[i], layer, row, column).astype(jnp.float32) + term(i, layer, 2, row, column)).astype(jnp.bfloat16)

        each_tile(runs, add_first)
        sum_copy(at, 1).start()

    @pl.loop(1, n - 2)
    def _(step):
        for at, (rightward, _, _, runs) in enumerate(plan.sums):
            sum_copy(at, step).wait_recv()
            wait_loads(runs, step + 2)

            def add(layer, i, row, column, tile):
                sums[step, tile] = (sums[step, tile].astype(jnp.float32) + term(i, layer, step + 2, row, column)).astype(jnp.bfloat16)

            each_tile(runs, add)
            sum_copy(at, step + 1).start()

    for i in range(3):
        own_load(i).wait()
        for copy in moment_load(i):
            copy.wait()

    for at, (rightward, _, _, runs) in enumerate(plan.sums):
        sum_copy(at, n - 2).wait_recv()
        wait_loads(runs, n)

        def take_step(layer, i, row, column, tile):
            g = (sums[n - 2, tile].astype(jnp.float32) + term(i, layer, n, row, column)).astype(jnp.bfloat16).astype(jnp.float32)
            place = (layer, pl.ds(pl.multiple_of(row, ROWS), ROWS), pl.ds(column, LANES))
            w, m, v = adamw(own[i][place].astype(jnp.float32), new_m[i][place], new_v[i][place], g)
            news[me, tile] = w
            new_w[i][layer, pl.ds(pl.multiple_of(me * plan.block[i] + row, ROWS), ROWS), pl.ds(column, LANES)] = w
            new_m[i][place] = m
            new_v[i][place] = v

        each_tile(runs, take_step)
        out_copy(at, 0).start()

    for i, layer in every:
        first_copy(i, layer).wait_send()

    def deal(at, step):
        rightward, _, _, runs = plan.news[at]
        device = behind(rightward, step + 1)

        def move(layer, i, row, column, tile):
            new_w[i][layer, pl.ds(pl.multiple_of(device * plan.block[i] + row, ROWS), ROWS), pl.ds(column, LANES)] = news[device, tile]

        each_tile(runs, move)

    @pl.loop(0, n - 2)
    def _(step):
        for at in range(len(plan.news)):
            out_copy(at, step).wait_recv()
            out_copy(at, step + 1).start()
            deal(at, step)
        for at in range(len(plan.news)):
            sum_copy(at, step + 1).wait_send()

        @pl.when(step > 0)
        def _():
            for at in range(len(plan.news)):
                out_copy(at, step - 1).wait_send()

    for at in range(len(plan.news)):
        out_copy(at, n - 3).wait_send()
    for at in range(len(plan.news)):
        out_copy(at, n - 2).wait_recv()
        deal(at, n - 2)
    for at in range(len(plan.news)):
        out_copy(at, n - 2).wait_send()


def put(*refs):
    count = len(refs) // 2
    copies = [pltpu.make_async_copy(refs[i], refs[count + i], refs[-1].at[i]) for i in range(count)]
    for copy in copies:
        copy.start()
    for copy in copies:
        copy.wait()


def solution(mesh):
    n = mesh.shape[AXIS]

    def step(*arrays):
        terms, weights, m, v = (arrays[i : i + 3] for i in (0, 3, 6, 9))
        plan = Plan([one.shape for one in m])
        layers = plan.layers
        dma, kind = pltpu.SemaphoreType.DMA, weights[0].dtype
        arrays = [pltpu.with_memory_space_constraint(one, pltpu.HBM) for one in arrays]
        new = pl.pallas_call(
            functools.partial(kernel, n, plan),
            out_shape=tuple(pltpu.VMEM(one.shape, one.dtype) for one in weights + m + v),
            in_specs=[pl.BlockSpec(memory_space=pltpu.HBM)] * 12,
            out_specs=(pl.BlockSpec(memory_space=pltpu.VMEM),) * 9,
            scratch_shapes=[pltpu.VMEM(w.shape, kind) for w in weights]
            + [pltpu.VMEM(one.shape, kind) for one in m + m]
            + [pltpu.VMEM((n - 1, plan.tiles, ROWS, LANES), kind), pltpu.VMEM((n, plan.tiles, ROWS, LANES), kind)]
            + [pltpu.SemaphoreType.REGULAR((2,)), dma((3, layers, n - 1)), dma((3,)), dma((3,)), dma((3,))]
            + [dma((3, layers))] * 2
            + [dma((n - 2, len(plan.sums)))] * 2
            + [dma((n - 1, len(plan.news)))] * 2,
            compiler_params=pltpu.CompilerParams(collective_id=0, has_side_effects=True, vmem_limit_bytes=40 * 2**20),
        )(*arrays)
        new = [pltpu.with_memory_space_constraint(one, pltpu.VMEM) for one in new]
        return pl.pallas_call(
            put,
            out_shape=tuple(pltpu.HBM(one.shape, one.dtype) for one in weights + m + v),
            in_specs=[pl.BlockSpec(memory_space=pltpu.VMEM)] * 9,
            out_specs=(pl.BlockSpec(memory_space=pltpu.HBM),) * 9,
            scratch_shapes=[dma((9,))],
            compiler_params=pltpu.CompilerParams(vmem_limit_bytes=2**20),
        )(*new)

    all_of, part = P(None, None, None), P(None, AXIS, None)
    return jax.shard_map(
        step,
        mesh=mesh,
        in_specs=(P(("rep", AXIS), None, None, None),) * 3 + (all_of,) * 3 + (part,) * 6,
        out_specs=(P("rep", None, None),) * 3 + (P("rep", AXIS, None),) * 6,
        check_vma=False,
    )
```

```python
import functools

import jax
import jax.numpy as jnp
from jax import lax
from jax.experimental import pallas as pl
from jax.experimental.pallas import tpu as pltpu
from jax.sharding import PartitionSpec as P

AXIS = "dp"
MESH = pl.DeviceIdType.MESH
ROWS, LANES = 16, 128
SHORTER = 3

def adamw(w, m, v, g):
    m = 0.9 * m + 0.1 * g
    v = 0.95 * v + 0.05 * g * g
    step = m * lax.rsqrt(v + 1e-8) + 0.1 * w
    return (w - 0.02 * step).astype(jnp.bfloat16), m, v

class Plan:
    def __init__(self, shapes):
        self.layers = shapes[0][0]
        self.block = [shape[1] for shape in shapes]
        self.wide = [shape[2] // LANES for shape in shapes]
        half = self.layers // 2
        order = sorted(range(len(shapes)), key=lambda i: (self.wide[i], i))
        bands, tile = {}, 0
        for rightward in (False, True):
            bands[rightward] = []
            for layer in range(half) if rightward else range(half, self.layers):
                for i in order:
                    for row in range(self.block[i] // ROWS):
                        bands[rightward].append((layer, i, row, tile))
                        tile += self.wide[i]
        self.tiles = tile
        ways = []
        for rightward in (True, False):
            all_of, start = bands[rightward], bands[rightward][0][3]
            at = next(k for k, band in enumerate(all_of) if 2 * (band[3] - start) >= self.tiles // 2)
            ways.append([(rightward, part) for part in (all_of[:at], all_of[at:])])
        self.copies = [
            (rightward, part[0][3], sum(self.wide[i] for _, i, _, _ in part), self.runs(part))
            for pair in zip(*ways, strict=True)
            for rightward, part in pair
        ]
        self.left_out = sum(self.wide[i] for _, i, _, _ in bands[True][-SHORTER:])

    def runs(self, bands):
        runs = []
        for layer, i, row, tile in bands:
            if runs and runs[-1][:2] == [layer, i]:
                runs[-1][3] += 1
            else:
                runs.append([layer, i, row, 1, tile])
        return runs

def kernel(n, plan, *refs):
    terms, weights, ms, vs = (refs[i : i + 3] for i in (0, 3, 6, 9))
    new_w, new_m, new_v, held, own, first = (refs[i : i + 3] for i in (12, 15, 18, 21, 24, 27))
    sums, news, entered, held_sem, own_sem, m_sem, v_sem, first_send, first_recv, sum_send, sum_recv, out_send, out_recv, end_send, end_recv = refs[30:]
    me = lax.axis_index(AXIS)
    right, left = lax.rem(me + 1, n), lax.rem(me + n - 1, n)
    half = plan.layers // 2
    every = [(i, layer) for i in sorted(range(3), key=lambda i: (plan.wide[i], i)) for pair in range(half) for layer in (pair, half + pair)]

    def behind(rightward, steps):
        return lax.rem(me + n - steps if rightward else me + steps, n)

    def rows(i, device):
        return pl.ds(pl.multiple_of(device * plan.block[i], ROWS), plan.block[i])

    def send(rightward, source, target, send_sem, recv_sem):
        return pltpu.make_async_remote_copy(
            src_ref=source,
            dst_ref=target,
            send_sem=send_sem,
            recv_sem=recv_sem,
            device_id={AXIS: right if rightward else left},
            device_id_type=MESH,
        )

    def first_copy(i, layer):
        rightward = layer < half
        source = terms[i].at[0, layer, rows(i, behind(rightward, 1))]
        return send(rightward, source, first[i].at[layer], first_send.at[i, layer], first_recv.at[i, layer])

    def sum_copy(at, step):
        rightward, tile, count, _ = plan.copies[at]
        part = pl.ds(tile, count)
        return send(rightward, sums.at[step - 1, part], sums.at[step, part], sum_send.at[step - 1, at], sum_recv.at[step - 1, at])

    def out_copy(at, step, left_out=0):
        rightward, tile, count, _ = plan.copies[at]
        count -= left_out
        piece = news.at[behind(rightward, step), pl.ds(tile, count)]
        return send(rightward, piece, piece, out_send.at[step, at], out_recv.at[step, at])

    def end_copy(at):
        rightward, tile, count, _ = plan.copies[at]
        piece = news.at[me, pl.ds(tile + count - plan.left_out, plan.left_out)]
        return send(not rightward, piece, piece, end_send.at[int(rightward)], end_recv.at[int(rightward)])

    def load(i, layer, steps):
        part = rows(i, behind(layer < half, steps))
        return pltpu.make_async_copy(terms[i].at[0, layer, part], held[i].at[layer, part], held_sem.at[i, layer, steps - 2])

    def own_load(i):
        return pltpu.make_async_copy(weights[i].at[:, rows(i, me)], own[i], own_sem.at[i])

    def moment_load(i):
        return (pltpu.make_async_copy(ms[i], new_m[i], m_sem.at[i]), pltpu.make_async_copy(vs[i], new_v[i], v_sem.at[i]))

    def each_tile(runs, body):
        for layer, i, row, count, tile in runs:

            @pl.loop(0, count)
            def _(k, layer=layer, i=i, row=row, tile=tile):
                for column in range(plan.wide[i]):
                    body(layer, i, (row + k) * ROWS, column * LANES, tile + k * plan.wide[i] + column)

    def tile_of(ref, layer, row, column):
        return ref[layer, pl.ds(pl.multiple_of(row, ROWS), ROWS), pl.ds(column, LANES)]

    def term(i, layer, steps, row, column):
        device = behind(layer < half, steps)
        return tile_of(held[i], layer, device * plan.block[i] + row, column).astype(jnp.float32)

    barrier = pltpu.get_barrier_semaphore()

    @pl.when(me < n - 2)
    def _():
        pl.semaphore_signal(barrier, inc=1, device_id={AXIS: right}, device_id_type=MESH)

    @pl.when((me == 0) | (me == n - 1))
    def _():
        pl.semaphore_signal(barrier, inc=1, device_id={AXIS: left}, device_id_type=MESH)

    def start(rightward):
        for i, layer in every:
            if (layer < half) == rightward:
                first_copy(i, layer).start()

    @pl.when(me > 0)
    def _():
        pl.semaphore_wait(barrier, 1 + (me == n - 2).astype(jnp.int32))

    @pl.when((me > 0) & (me < n - 1))
    def _():
        pl.semaphore_signal(entered.at[1], inc=1, device_id={AXIS: left}, device_id_type=MESH)
        start(False)

    @pl.when(me >= n - 2)
    def _():
        pl.semaphore_signal(entered.at[0], inc=1, device_id={AXIS: right}, device_id_type=MESH)
        start(True)

    @pl.when(me < n - 2)
    def _():
        pl.semaphore_wait(entered.at[1], 1)
        start(True)

    @pl.when((me == 0) | (me == n - 1))
    def _():
        pl.semaphore_wait(entered.at[0], 1)
        start(False)

    for steps in range(2, n + 1):
        for i, layer in every:
            load(i, layer, steps).start()
    for i in range(3):
        own_load(i).start()
        for copy in moment_load(i):
            copy.start()

    def wait_loads(runs, steps):
        for layer, i, row, _, _ in runs:
            if row == 0:
                load(i, layer, steps).wait()

    arrived = set()
    for at, (rightward, _, _, runs) in enumerate(plan.copies):
        for layer, i, row, _, _ in runs:
            if (i, layer) not in arrived:
                first_copy(i, layer).wait_recv()
                arrived.add((i, layer))
        wait_loads(runs, 2)

        def add_first(layer, i, row, column, tile):
            sums[0, tile] = (tile_of(first[i], layer, row, column).astype(jnp.float32) + term(i, layer, 2, row, column)).astype(jnp.bfloat16)

        each_tile(runs, add_first)
        sum_copy(at, 1).start()

    @pl.loop(1, n - 2)
    def _(step):
        for at, (rightward, _, _, runs) in enumerate(plan.copies):
            sum_copy(at, step).wait_recv()
            wait_loads(runs, step + 2)

            def add(layer, i, row, column, tile):
                sums[step, tile] = (sums[step, tile].astype(jnp.float32) + term(i, layer, step + 2, row, column)).astype(jnp.bfloat16)

            each_tile(runs, add)
            sum_copy(at, step + 1).start()

    for i in range(3):
        own_load(i).wait()
        for copy in moment_load(i):
            copy.wait()

    for at, (rightward, _, _, runs) in enumerate(plan.copies):
        sum_copy(at, n - 2).wait_recv()
        wait_loads(runs, n)

        def take_step(layer, i, row, column, tile):
            g = (sums[n - 2, tile].astype(jnp.float32) + term(i, layer, n, row, column)).astype(jnp.bfloat16).astype(jnp.float32)
            place = (layer, pl.ds(pl.multiple_of(row, ROWS), ROWS), pl.ds(column, LANES))
            w, m, v = adamw(own[i][place].astype(jnp.float32), new_m[i][place], new_v[i][place], g)
            news[me, tile] = w
            new_w[i][layer, pl.ds(pl.multiple_of(me * plan.block[i] + row, ROWS), ROWS), pl.ds(column, LANES)] = w
            new_m[i][place] = m
            new_v[i][place] = v

        each_tile(runs, take_step)
        out_copy(at, 0).start()

    for i, layer in every:
        first_copy(i, layer).wait_send()

    def deal(at, step):
        rightward, _, _, runs = plan.copies[at]
        device = behind(rightward, step + 1)

        def move(layer, i, row, column, tile):
            new_w[i][layer, pl.ds(pl.multiple_of(device * plan.block[i] + row, ROWS), ROWS), pl.ds(column, LANES)] = news[device, tile]

        each_tile(runs, move)

    @pl.loop(0, n - 3)
    def _(step):
        for at in range(len(plan.copies)):
            out_copy(at, step).wait_recv()
            out_copy(at, step + 1).start()
            deal(at, step)
        for at in range(len(plan.copies)):
            sum_copy(at, step + 1).wait_send()

        @pl.when(step > 0)
        def _():
            for at in range(len(plan.copies)):
                out_copy(at, step - 1).wait_send()

    ends = range(len(plan.copies) - 2, len(plan.copies))

    def last(at, shorter, do):
        if at not in ends:
            do(out_copy(at, n - 2))
            return
        pl.when(shorter)(lambda: do(out_copy(at, n - 2, plan.left_out)))
        pl.when(jnp.logical_not(shorter))(lambda: do(out_copy(at, n - 2)))

    def sends_shorter(at):
        return me == (n - 1 if plan.copies[at][0] else 0)

    def gets_shorter(at):
        return me == (0 if plan.copies[at][0] else n - 1)

    def sends_end(at):
        return me == (1 if plan.copies[at][0] else n - 2)

    for at in range(len(plan.copies)):
        out_copy(at, n - 3).wait_recv()
        last(at, sends_shorter(at), lambda copy: copy.start())
        if at in ends:
            pl.when(sends_end(at))(lambda at=at: end_copy(at).start())
        deal(at, n - 3)
    for at in range(len(plan.copies)):
        sum_copy(at, n - 2).wait_send()
        out_copy(at, n - 4).wait_send()
        out_copy(at, n - 3).wait_send()
    for at in range(len(plan.copies)):
        last(at, gets_shorter(at), lambda copy: copy.wait_recv())
        if at in ends:
            pl.when(gets_shorter(at))(lambda at=at: end_copy(at).wait_recv())
        deal(at, n - 2)
    for at in range(len(plan.copies)):
        last(at, sends_shorter(at), lambda copy: copy.wait_send())
        if at in ends:
            pl.when(sends_end(at))(lambda at=at: end_copy(at).wait_send())

def put(*refs):
    count = len(refs) // 2
    copies = [pltpu.make_async_copy(refs[i], refs[count + i], refs[-1].at[i]) for i in range(count)]
    for copy in copies:
        copy.start()
    for copy in copies:
        copy.wait()

def solution(mesh):
    n = mesh.shape[AXIS]

    def step(*arrays):
        terms, weights, m, v = (arrays[i : i + 3] for i in (0, 3, 6, 9))
        plan = Plan([one.shape for one in m])
        layers = plan.layers
        dma, kind = pltpu.SemaphoreType.DMA, weights[0].dtype
        arrays = [pltpu.with_memory_space_constraint(one, pltpu.HBM) for one in arrays]
        new = pl.pallas_call(
            functools.partial(kernel, n, plan),
            out_shape=tuple(pltpu.VMEM(one.shape, one.dtype) for one in weights + m + v),
            in_specs=[pl.BlockSpec(memory_space=pltpu.HBM)] * 12,
            out_specs=(pl.BlockSpec(memory_space=pltpu.VMEM),) * 9,
            scratch_shapes=[pltpu.VMEM(w.shape, kind) for w in weights]
            + [pltpu.VMEM(one.shape, kind) for one in m + m]
            + [pltpu.VMEM((n - 1, plan.tiles, ROWS, LANES), kind), pltpu.VMEM((n, plan.tiles, ROWS, LANES), kind)]
            + [pltpu.SemaphoreType.REGULAR((2,)), dma((3, layers, n - 1)), dma((3,)), dma((3,)), dma((3,))]
            + [dma((3, layers))] * 2
            + [dma((n - 2, len(plan.copies)))] * 2
            + [dma((n - 1, len(plan.copies)))] * 2
            + [dma((2,))] * 2,
            compiler_params=pltpu.CompilerParams(collective_id=0, has_side_effects=True, vmem_limit_bytes=40 * 2**20),
        )(*arrays)
        new = [pltpu.with_memory_space_constraint(one, pltpu.VMEM) for one in new]
        return pl.pallas_call(
            put,
            out_shape=tuple(pltpu.HBM(one.shape, one.dtype) for one in weights + m + v),
            in_specs=[pl.BlockSpec(memory_space=pltpu.VMEM)] * 9,
            out_specs=(pl.BlockSpec(memory_space=pltpu.HBM),) * 9,
            scratch_shapes=[dma((9,))],
            compiler_params=pltpu.CompilerParams(vmem_limit_bytes=2**20),
        )(*new)

    all_of, part = P(None, None, None), P(None, AXIS, None)
    return jax.shard_map(
        step,
        mesh=mesh,
        in_specs=(P(("rep", AXIS), None, None, None),) * 3 + (all_of,) * 3 + (part,) * 6,
        out_specs=(P("rep", None, None),) * 3 + (P("rep", AXIS, None),) * 6,
        check_vma=False,
    )
```

```python
import functools

import jax
import jax.numpy as jnp
from jax import lax
from jax.experimental import pallas as pl
from jax.experimental.pallas import tpu as pltpu
from jax.sharding import PartitionSpec as P

AXIS = "dp"
MESH = pl.DeviceIdType.MESH
ROWS, LANES = 16, 128
SHORTER = 4

def adamw(w, m, v, g):
    m = 0.9 * m + 0.1 * g
    v = 0.95 * v + 0.05 * g * g
    step = m * lax.rsqrt(v + 1e-8) + 0.1 * w
    return (w - 0.02 * step).astype(jnp.bfloat16), m, v

class Plan:
    def __init__(self, shapes):
        self.layers = shapes[0][0]
        self.block = [shape[1] for shape in shapes]
        self.wide = [shape[2] // LANES for shape in shapes]
        half = self.layers // 2
        order = sorted(range(len(shapes)), key=lambda i: (self.wide[i], i))
        bands, tile = {}, 0
        for rightward in (False, True):
            bands[rightward] = []
            for layer in range(half) if rightward else range(half, self.layers):
                for i in order:
                    for row in range(self.block[i] // ROWS):
                        bands[rightward].append((layer, i, row, tile))
                        tile += self.wide[i]
        self.tiles = tile
        ways = []
        for rightward in (True, False):
            all_of, start = bands[rightward], bands[rightward][0][3]
            at = next(k for k, band in enumerate(all_of) if 2 * (band[3] - start) >= self.tiles // 2)
            ways.append([(rightward, part) for part in (all_of[:at], all_of[at:])])
        self.copies = [
            (rightward, part[0][3], sum(self.wide[i] for _, i, _, _ in part), self.runs(part))
            for pair in zip(*ways, strict=True)
            for rightward, part in pair
        ]
        self.left_out = sum(self.wide[i] for _, i, _, _ in bands[True][-SHORTER:])

    def runs(self, bands):
        runs = []
        for layer, i, row, tile in bands:
            if runs and runs[-1][:2] == [layer, i]:
                runs[-1][3] += 1
            else:
                runs.append([layer, i, row, 1, tile])
        return runs

def kernel(n, plan, *refs):
    terms, weights, ms, vs = (refs[i : i + 3] for i in (0, 3, 6, 9))
    new_w, new_m, new_v, held, own, first = (refs[i : i + 3] for i in (12, 15, 18, 21, 24, 27))
    sums, news, entered, held_sem, own_sem, m_sem, v_sem, first_send, first_recv, sum_send, sum_recv, out_send, out_recv, end_send, end_recv = refs[30:]
    me = lax.axis_index(AXIS)
    right, left = lax.rem(me + 1, n), lax.rem(me + n - 1, n)
    half = plan.layers // 2
    every = [(i, layer) for i in sorted(range(3), key=lambda i: (plan.wide[i], i)) for pair in range(half) for layer in (pair, half + pair)]

    def behind(rightward, steps):
        return lax.rem(me + n - steps if rightward else me + steps, n)

    def rows(i, device):
        return pl.ds(pl.multiple_of(device * plan.block[i], ROWS), plan.block[i])

    def send(rightward, source, target, send_sem, recv_sem):
        return pltpu.make_async_remote_copy(
            src_ref=source,
            dst_ref=target,
            send_sem=send_sem,
            recv_sem=recv_sem,
            device_id={AXIS: right if rightward else left},
            device_id_type=MESH,
        )

    def first_copy(i, layer):
        rightward = layer < half
        source = terms[i].at[0, layer, rows(i, behind(rightward, 1))]
        return send(rightward, source, first[i].at[layer], first_send.at[i, layer], first_recv.at[i, layer])

    def sum_copy(at, step):
        rightward, tile, count, _ = plan.copies[at]
        part = pl.ds(tile, count)
        return send(rightward, sums.at[step - 1, part], sums.at[step, part], sum_send.at[step - 1, at], sum_recv.at[step - 1, at])

    def out_copy(at, step, left_out=0):
        rightward, tile, count, _ = plan.copies[at]
        count -= left_out
        piece = news.at[behind(rightward, step), pl.ds(tile, count)]
        return send(rightward, piece, piece, out_send.at[step, at], out_recv.at[step, at])

    def end_copy(at):
        rightward, tile, count, _ = plan.copies[at]
        piece = news.at[me, pl.ds(tile + count - plan.left_out, plan.left_out)]
        return send(not rightward, piece, piece, end_send.at[int(rightward)], end_recv.at[int(rightward)])

    def load(i, layer, steps):
        part = rows(i, behind(layer < half, steps))
        return pltpu.make_async_copy(terms[i].at[0, layer, part], held[i].at[layer, part], held_sem.at[i, layer, steps - 2])

    def own_load(i):
        return pltpu.make_async_copy(weights[i].at[:, rows(i, me)], own[i], own_sem.at[i])

    def moment_load(i):
        return (pltpu.make_async_copy(ms[i], new_m[i], m_sem.at[i]), pltpu.make_async_copy(vs[i], new_v[i], v_sem.at[i]))

    def each_tile(runs, body, unroll=False):
        for layer, i, row, count, tile in runs:

            @pl.loop(0, count, unroll=unroll)
            def _(k, layer=layer, i=i, row=row, tile=tile):
                for column in range(plan.wide[i]):
                    body(layer, i, (row + k) * ROWS, column * LANES, tile + k * plan.wide[i] + column)

    def tile_of(ref, layer, row, column):
        return ref[layer, pl.ds(pl.multiple_of(row, ROWS), ROWS), pl.ds(column, LANES)]

    def term(i, layer, steps, row, column):
        device = behind(layer < half, steps)
        return tile_of(held[i], layer, device * plan.block[i] + row, column).astype(jnp.float32)

    barrier = pltpu.get_barrier_semaphore()

    @pl.when(me < n - 2)
    def _():
        pl.semaphore_signal(barrier, inc=1, device_id={AXIS: right}, device_id_type=MESH)

    @pl.when((me == 0) | (me == n - 1))
    def _():
        pl.semaphore_signal(barrier, inc=1, device_id={AXIS: left}, device_id_type=MESH)

    def start(rightward):
        for i, layer in every:
            if (layer < half) == rightward:
                first_copy(i, layer).start()

    @pl.when(me > 0)
    def _():
        pl.semaphore_wait(barrier, 1 + (me == n - 2).astype(jnp.int32))

    @pl.when((me > 0) & (me < n - 1))
    def _():
        pl.semaphore_signal(entered.at[1], inc=1, device_id={AXIS: left}, device_id_type=MESH)
        start(False)

    @pl.when(me >= n - 2)
    def _():
        pl.semaphore_signal(entered.at[0], inc=1, device_id={AXIS: right}, device_id_type=MESH)
        start(True)

    @pl.when(me < n - 2)
    def _():
        pl.semaphore_wait(entered.at[1], 1)
        start(True)

    @pl.when((me == 0) | (me == n - 1))
    def _():
        pl.semaphore_wait(entered.at[0], 1)
        start(False)

    for steps in range(2, n + 1):
        for i, layer in every:
            load(i, layer, steps).start()
    for i in range(3):
        own_load(i).start()
        for copy in moment_load(i):
            copy.start()

    def wait_loads(runs, steps):
        for layer, i, row, _, _ in runs:
            if row == 0:
                load(i, layer, steps).wait()

    arrived = set()
    for at, (rightward, _, _, runs) in enumerate(plan.copies):
        for layer, i, row, _, _ in runs:
            if (i, layer) not in arrived:
                first_copy(i, layer).wait_recv()
                arrived.add((i, layer))
        wait_loads(runs, 2)

        def add_first(layer, i, row, column, tile):
            sums[0, tile] = (tile_of(first[i], layer, row, column).astype(jnp.float32) + term(i, layer, 2, row, column)).astype(jnp.bfloat16)

        each_tile(runs, add_first)
        sum_copy(at, 1).start()

    @pl.loop(1, n - 2)
    def _(step):
        for at, (rightward, _, _, runs) in enumerate(plan.copies):
            sum_copy(at, step).wait_recv()
            wait_loads(runs, step + 2)

            def add(layer, i, row, column, tile):
                sums[step, tile] = (sums[step, tile].astype(jnp.float32) + term(i, layer, step + 2, row, column)).astype(jnp.bfloat16)

            each_tile(runs, add)
            sum_copy(at, step + 1).start()

    for i in range(3):
        own_load(i).wait()
        for copy in moment_load(i):
            copy.wait()

    for at, (rightward, _, _, runs) in enumerate(plan.copies):
        sum_copy(at, n - 2).wait_recv()
        wait_loads(runs, n)

        def take_step(layer, i, row, column, tile):
            g = (sums[n - 2, tile].astype(jnp.float32) + term(i, layer, n, row, column)).astype(jnp.bfloat16).astype(jnp.float32)
            place = (layer, pl.ds(pl.multiple_of(row, ROWS), ROWS), pl.ds(column, LANES))
            w, m, v = adamw(own[i][place].astype(jnp.float32), new_m[i][place], new_v[i][place], g)
            news[me, tile] = w
            new_w[i][layer, pl.ds(pl.multiple_of(me * plan.block[i] + row, ROWS), ROWS), pl.ds(column, LANES)] = w
            new_m[i][place] = m
            new_v[i][place] = v

        each_tile(runs, take_step)
        out_copy(at, 0).start()

    for i, layer in every:
        first_copy(i, layer).wait_send()

    def deal(at, step, unroll=False):
        rightward, _, _, runs = plan.copies[at]
        device = behind(rightward, step + 1)

        def move(layer, i, row, column, tile):
            new_w[i][layer, pl.ds(pl.multiple_of(device * plan.block[i] + row, ROWS), ROWS), pl.ds(column, LANES)] = news[device, tile]

        each_tile(runs, move, unroll)

    @pl.loop(0, n - 3)
    def _(step):
        for at in range(len(plan.copies)):
            out_copy(at, step).wait_recv()
            out_copy(at, step + 1).start()
            deal(at, step)
        for at in range(len(plan.copies)):
            sum_copy(at, step + 1).wait_send()

        @pl.when(step > 0)
        def _():
            for at in range(len(plan.copies)):
                out_copy(at, step - 1).wait_send()

    ends = range(len(plan.copies) - 2, len(plan.copies))

    def last(at, shorter, do):
        if at not in ends:
            do(out_copy(at, n - 2))
            return
        pl.when(shorter)(lambda: do(out_copy(at, n - 2, plan.left_out)))
        pl.when(jnp.logical_not(shorter))(lambda: do(out_copy(at, n - 2)))

    def sends_shorter(at):
        return me == (n - 1 if plan.copies[at][0] else 0)

    def gets_shorter(at):
        return me == (0 if plan.copies[at][0] else n - 1)

    def sends_end(at):
        return me == (1 if plan.copies[at][0] else n - 2)

    for at in range(len(plan.copies)):
        out_copy(at, n - 3).wait_recv()
        last(at, sends_shorter(at), lambda copy: copy.start())
        if at in ends:
            pl.when(sends_end(at))(lambda at=at: end_copy(at).start())
        deal(at, n - 3)
    for at in range(len(plan.copies)):
        sum_copy(at, n - 2).wait_send()
        out_copy(at, n - 4).wait_send()
        out_copy(at, n - 3).wait_send()
    for at in range(len(plan.copies)):
        last(at, gets_shorter(at), lambda copy: copy.wait_recv())
        if at in ends:
            pl.when(gets_shorter(at))(lambda at=at: end_copy(at).wait_recv())
        deal(at, n - 2, True)
    for at in range(len(plan.copies)):
        last(at, sends_shorter(at), lambda copy: copy.wait_send())
        if at in ends:
            pl.when(sends_end(at))(lambda at=at: end_copy(at).wait_send())

def put(*refs):
    count = len(refs) // 2
    copies = [pltpu.make_async_copy(refs[i], refs[count + i], refs[-1].at[i]) for i in range(count)]
    for copy in copies:
        copy.start()
    for copy in copies:
        copy.wait()

def solution(mesh):
    n = mesh.shape[AXIS]

    def step(*arrays):
        terms, weights, m, v = (arrays[i : i + 3] for i in (0, 3, 6, 9))
        plan = Plan([one.shape for one in m])
        layers = plan.layers
        dma, kind = pltpu.SemaphoreType.DMA, weights[0].dtype
        arrays = [pltpu.with_memory_space_constraint(one, pltpu.HBM) for one in arrays]
        new = pl.pallas_call(
            functools.partial(kernel, n, plan),
            out_shape=tuple(pltpu.VMEM(one.shape, one.dtype) for one in weights + m + v),
            in_specs=[pl.BlockSpec(memory_space=pltpu.HBM)] * 12,
            out_specs=(pl.BlockSpec(memory_space=pltpu.VMEM),) * 9,
            scratch_shapes=[pltpu.VMEM(w.shape, kind) for w in weights]
            + [pltpu.VMEM(one.shape, kind) for one in m + m]
            + [pltpu.VMEM((n - 1, plan.tiles, ROWS, LANES), kind), pltpu.VMEM((n, plan.tiles, ROWS, LANES), kind)]
            + [pltpu.SemaphoreType.REGULAR((2,)), dma((3, layers, n - 1)), dma((3,)), dma((3,)), dma((3,))]
            + [dma((3, layers))] * 2
            + [dma((n - 2, len(plan.copies)))] * 2
            + [dma((n - 1, len(plan.copies)))] * 2
            + [dma((2,))] * 2,
            compiler_params=pltpu.CompilerParams(collective_id=0, has_side_effects=True, vmem_limit_bytes=40 * 2**20),
        )(*arrays)
        new = [pltpu.with_memory_space_constraint(one, pltpu.VMEM) for one in new]
        return pl.pallas_call(
            put,
            out_shape=tuple(pltpu.HBM(one.shape, one.dtype) for one in weights + m + v),
            in_specs=[pl.BlockSpec(memory_space=pltpu.VMEM)] * 9,
            out_specs=(pl.BlockSpec(memory_space=pltpu.HBM),) * 9,
            scratch_shapes=[dma((9,))],
            compiler_params=pltpu.CompilerParams(vmem_limit_bytes=2**20),
        )(*new)

    all_of, part = P(None, None, None), P(None, AXIS, None)
    return jax.shard_map(
        step,
        mesh=mesh,
        in_specs=(P(("rep", AXIS), None, None, None),) * 3 + (all_of,) * 3 + (part,) * 6,
        out_specs=(P("rep", None, None),) * 3 + (P("rep", AXIS, None),) * 6,
        check_vma=False,
    )
```

```python
import functools

import jax
import jax.numpy as jnp
from jax import lax
from jax.experimental import pallas as pl
from jax.experimental.pallas import tpu as pltpu
from jax.sharding import PartitionSpec as P

AXIS = "dp"
MESH = pl.DeviceIdType.MESH
ROWS, LANES = 16, 128
LEFT_OUT = {True: 38, False: 16}
AROUND = 80

def adamw(w, m, v, g):
    m = 0.9 * m + 0.1 * g
    v = 0.95 * v + 0.05 * g * g
    step = m * lax.rsqrt(v + 1e-8) + 0.1 * w
    return (w - 0.02 * step).astype(jnp.bfloat16), m, v

class Plan:
    def __init__(self, shapes):
        self.layers = shapes[0][0]
        self.block = [shape[1] for shape in shapes]
        self.wide = [shape[2] // LANES for shape in shapes]
        half = self.layers // 2
        self.order = sorted(range(len(shapes)), key=lambda i: (self.wide[i], i))
        bands, tile = {}, 0
        for rightward in (False, True):
            bands[rightward] = []
            for layer in range(half) if rightward else range(half, self.layers):
                for i in self.order:
                    for row in range(self.block[i] // ROWS):
                        bands[rightward].append((layer, i, row, tile))
                        tile += self.wide[i]
        self.tiles = tile
        ways = []
        for rightward in (True, False):
            all_of, start = bands[rightward], bands[rightward][0][3]
            at = next(k for k, band in enumerate(all_of) if 2 * (band[3] - start) >= self.tiles // 2)
            ways.append([(rightward, part) for part in (all_of[:at], all_of[at:])])
        self.copies = [
            (rightward, part[0][3], sum(self.wide[i] for _, i, _, _ in part), self.runs(part))
            for pair in zip(*ways, strict=True)
            for rightward, part in pair
        ]

    def runs(self, bands):
        runs = []
        for layer, i, row, tile in bands:
            if runs and runs[-1][:2] == [layer, i]:
                runs[-1][3] += 1
            else:
                runs.append([layer, i, row, 1, tile])
        return runs

def kernel(n, plan, *refs):
    terms, weights, ms, vs = (refs[i : i + 3] for i in (0, 3, 6, 9))
    new_w, new_m, new_v, held, own, first = (refs[i : i + 3] for i in (12, 15, 18, 21, 24, 27))
    around, around_send, around_recv = refs[-3:]
    sums, news, entered, held_sem, own_sem, m_sem, v_sem, first_send, first_recv, sum_send, sum_recv, out_send, out_recv, end_send, end_recv = refs[30:-3]
    me = lax.axis_index(AXIS)
    right, left = lax.rem(me + 1, n), lax.rem(me + n - 1, n)
    half = plan.layers // 2
    every = [(i, layer) for i in plan.order for pair in range(half) for layer in (pair, half + pair)]

    def behind(rightward, steps):
        return lax.rem(me + n - steps if rightward else me + steps, n)

    def rows(i, device):
        return pl.ds(pl.multiple_of(device * plan.block[i], ROWS), plan.block[i])

    def send(rightward, source, target, send_sem, recv_sem):
        return pltpu.make_async_remote_copy(
            src_ref=source,
            dst_ref=target,
            send_sem=send_sem,
            recv_sem=recv_sem,
            device_id={AXIS: right if rightward else left},
            device_id_type=MESH,
        )

    def first_copy(i, layer, skip=0):
        rightward, count = layer < half, plan.block[i] - skip
        source = terms[i].at[0, layer, pl.ds(pl.multiple_of(behind(rightward, 1) * plan.block[i] + skip, ROWS), count)]
        return send(rightward, source, first[i].at[layer, pl.ds(skip, count)], first_send.at[i, layer], first_recv.at[i, layer])

    split = plan.order[0], half
    splits, gets_rest, gets_around = me <= 1, (me == 0) | (me == n - 1), (me == 1) | (me == 2)

    def around_copy():
        i, layer = split
        source = terms[i].at[0, layer, pl.ds(pl.multiple_of(behind(False, 1) * plan.block[i], ROWS), AROUND)]
        return send(True, source, around, around_send, around_recv)

    def either(shorter, short, full, do):
        pl.when(shorter)(lambda: do(short()))
        pl.when(jnp.logical_not(shorter))(lambda: do(full()))

    def first_of(i, layer, shorter, do):
        if (i, layer) == split:
            either(shorter, lambda: first_copy(i, layer, AROUND), lambda: first_copy(i, layer), do)
        else:
            do(first_copy(i, layer))

    def sum_copy(at, step):
        rightward, tile, count, _ = plan.copies[at]
        part = pl.ds(tile, count)
        return send(rightward, sums.at[step - 1, part], sums.at[step, part], sum_send.at[step - 1, at], sum_recv.at[step - 1, at])

    def out_copy(at, step, left_out=0):
        rightward, tile, count, _ = plan.copies[at]
        count -= left_out
        piece = news.at[behind(rightward, step), pl.ds(tile, count)]
        return send(rightward, piece, piece, out_send.at[step, at], out_recv.at[step, at])

    def end_copy(at):
        rightward, tile, count, _ = plan.copies[at]
        piece = news.at[me, pl.ds(tile + count - LEFT_OUT[rightward], LEFT_OUT[rightward])]
        return send(not rightward, piece, piece, end_send.at[int(rightward)], end_recv.at[int(rightward)])

    def load(i, layer, steps):
        part = rows(i, behind(layer < half, steps))
        return pltpu.make_async_copy(terms[i].at[0, layer, part], held[i].at[layer, part], held_sem.at[i, layer, steps - 2])

    def own_load(i):
        return pltpu.make_async_copy(weights[i].at[:, rows(i, me)], own[i], own_sem.at[i])

    def moment_load(i):
        return (pltpu.make_async_copy(ms[i], new_m[i], m_sem.at[i]), pltpu.make_async_copy(vs[i], new_v[i], v_sem.at[i]))

    def each_tile(runs, body, unroll=False):
        for layer, i, row, count, tile in runs:

            @pl.loop(0, count, unroll=unroll)
            def _(k, layer=layer, i=i, row=row, tile=tile):
                for column in range(plan.wide[i]):
                    body(layer, i, (row + k) * ROWS, column * LANES, tile + k * plan.wide[i] + column)

    def tile_of(ref, layer, row, column):
        return ref[layer, pl.ds(pl.multiple_of(row, ROWS), ROWS), pl.ds(column, LANES)]

    def term(i, layer, steps, row, column):
        device = behind(layer < half, steps)
        return tile_of(held[i], layer, device * plan.block[i] + row, column).astype(jnp.float32)

    barrier = pltpu.get_barrier_semaphore()

    @pl.when(me < n - 2)
    def _():
        pl.semaphore_signal(barrier, inc=1, device_id={AXIS: right}, device_id_type=MESH)

    @pl.when((me == 0) | (me == n - 1))
    def _():
        pl.semaphore_signal(barrier, inc=1, device_id={AXIS: left}, device_id_type=MESH)

    def start(rightward):
        for i, layer in every:
            if (layer < half) == rightward:
                first_of(i, layer, splits, lambda copy: copy.start())

    @pl.when(me > 0)
    def _():
        pl.semaphore_wait(barrier, 1 + (me == n - 2).astype(jnp.int32))

    @pl.when((me > 0) & (me < n - 1))
    def _():
        pl.semaphore_signal(entered.at[1], inc=1, device_id={AXIS: left}, device_id_type=MESH)
        start(False)

    @pl.when(me >= n - 2)
    def _():
        pl.semaphore_signal(entered.at[0], inc=1, device_id={AXIS: right}, device_id_type=MESH)
        start(True)

    @pl.when(me < n - 2)
    def _():
        pl.semaphore_wait(entered.at[1], 1)
        start(True)

    @pl.when(splits)
    def _():
        around_copy().start()

    @pl.when((me == 0) | (me == n - 1))
    def _():
        pl.semaphore_wait(entered.at[0], 1)
        start(False)

    @pl.when(gets_rest)
    def _():
        i, layer = split
        first[i][layer, pl.ds(0, AROUND)] = jnp.zeros((AROUND, first[i].shape[2]), first[i].dtype)

    @pl.when(jnp.logical_not(gets_around))
    def _():
        around[...] = jnp.zeros_like(around)

    for steps in range(2, n + 1):
        for i, layer in every:
            load(i, layer, steps).start()
    for i in range(3):
        own_load(i).start()
        for copy in moment_load(i):
            copy.start()

    def wait_loads(runs, steps):
        for layer, i, row, _, _ in runs:
            if row == 0:
                load(i, layer, steps).wait()

    arrived = set()
    for at, (rightward, _, _, runs) in enumerate(plan.copies):
        for layer, i, row, _, _ in runs:
            if (i, layer) not in arrived:
                first_of(i, layer, gets_rest, lambda copy: copy.wait_recv())
                arrived.add((i, layer))
        wait_loads(runs, 2)

        def add_first(layer, i, row, column, tile):
            sums[0, tile] = (tile_of(first[i], layer, row, column).astype(jnp.float32) + term(i, layer, 2, row, column)).astype(jnp.bfloat16)

        each_tile(runs, add_first)
        sum_copy(at, 1).start()

    @pl.loop(1, n - 2)
    def _(step):
        for at, (rightward, _, _, runs) in enumerate(plan.copies):
            sum_copy(at, step).wait_recv()
            wait_loads(runs, step + 2)

            def add(layer, i, row, column, tile):
                sums[step, tile] = (sums[step, tile].astype(jnp.float32) + term(i, layer, step + 2, row, column)).astype(jnp.bfloat16)

            each_tile(runs, add)
            sum_copy(at, step + 1).start()

    for i in range(3):
        own_load(i).wait()
        for copy in moment_load(i):
            copy.wait()

    for at, (rightward, _, _, runs) in enumerate(plan.copies):
        sum_copy(at, n - 2).wait_recv()
        wait_loads(runs, n)

        def take_step(layer, i, row, column, tile, more=None):
            g = sums[n - 2, tile].astype(jnp.float32) + term(i, layer, n, row, column)
            if more is not None:
                g += more[pl.ds(pl.multiple_of(row, ROWS), ROWS), pl.ds(column, LANES)].astype(jnp.float32)
            g = g.astype(jnp.bfloat16).astype(jnp.float32)
            place = (layer, pl.ds(pl.multiple_of(row, ROWS), ROWS), pl.ds(column, LANES))
            w, m, v = adamw(own[i][place].astype(jnp.float32), new_m[i][place], new_v[i][place], g)
            news[me, tile] = w
            new_w[i][layer, pl.ds(pl.multiple_of(me * plan.block[i] + row, ROWS), ROWS), pl.ds(column, LANES)] = w
            new_m[i][place] = m
            new_v[i][place] = v

        for run in runs:
            layer, i, row, count, tile = run
            if (i, layer) == split and row == 0:
                pl.when(gets_around)(lambda: around_copy().wait_recv())
                part = AROUND // ROWS
                each_tile([(layer, i, row, part, tile)], functools.partial(take_step, more=around))
                run = (layer, i, row + part, count - part, tile + part * plan.wide[i])
            each_tile([run], take_step)
        out_copy(at, 0).start()

    for i, layer in every:
        first_of(i, layer, splits, lambda copy: copy.wait_send())
    pl.when(splits)(lambda: around_copy().wait_send())

    def deal(at, step, unroll=False):
        rightward, _, _, runs = plan.copies[at]
        device = behind(rightward, step + 1)

        def move(layer, i, row, column, tile):
            new_w[i][layer, pl.ds(pl.multiple_of(device * plan.block[i] + row, ROWS), ROWS), pl.ds(column, LANES)] = news[device, tile]

        each_tile(runs, move, unroll)

    @pl.loop(0, n - 3)
    def _(step):
        for at in range(len(plan.copies)):
            out_copy(at, step).wait_recv()
            out_copy(at, step + 1).start()
            deal(at, step)
        for at in range(len(plan.copies)):
            sum_copy(at, step + 1).wait_send()

        @pl.when(step > 0)
        def _():
            for at in range(len(plan.copies)):
                out_copy(at, step - 1).wait_send()

    ends = range(len(plan.copies) - 2, len(plan.copies))

    def last(at, shorter, do):
        if at not in ends:
            do(out_copy(at, n - 2))
            return
        left_out = LEFT_OUT[plan.copies[at][0]]
        either(shorter, lambda: out_copy(at, n - 2, left_out), lambda: out_copy(at, n - 2), do)

    def sends_shorter(at):
        return me == (n - 1 if plan.copies[at][0] else 0)

    def gets_shorter(at):
        return me == (0 if plan.copies[at][0] else n - 1)

    def sends_end(at):
        return me == (1 if plan.copies[at][0] else n - 2)

    for at in range(len(plan.copies)):
        out_copy(at, n - 3).wait_recv()
        last(at, sends_shorter(at), lambda copy: copy.start())
        if at in ends:
            pl.when(sends_end(at))(lambda at=at: end_copy(at).start())
        deal(at, n - 3)
    for at in range(len(plan.copies)):
        sum_copy(at, n - 2).wait_send()
        out_copy(at, n - 4).wait_send()
        out_copy(at, n - 3).wait_send()
    for at in range(len(plan.copies)):
        last(at, gets_shorter(at), lambda copy: copy.wait_recv())
        if at in ends:
            pl.when(gets_shorter(at))(lambda at=at: end_copy(at).wait_recv())
        deal(at, n - 2, True)
    for at in range(len(plan.copies)):
        last(at, sends_shorter(at), lambda copy: copy.wait_send())
        if at in ends:
            pl.when(sends_end(at))(lambda at=at: end_copy(at).wait_send())

def put(*refs):
    count = len(refs) // 2
    copies = [pltpu.make_async_copy(refs[i], refs[count + i], refs[-1].at[i]) for i in range(count)]
    for copy in copies:
        copy.start()
    for copy in copies:
        copy.wait()

def solution(mesh):
    n = mesh.shape[AXIS]

    def step(*arrays):
        terms, weights, m, v = (arrays[i : i + 3] for i in (0, 3, 6, 9))
        plan = Plan([one.shape for one in m])
        layers = plan.layers
        dma, kind = pltpu.SemaphoreType.DMA, weights[0].dtype
        arrays = [pltpu.with_memory_space_constraint(one, pltpu.HBM) for one in arrays]
        new = pl.pallas_call(
            functools.partial(kernel, n, plan),
            out_shape=tuple(pltpu.VMEM(one.shape, one.dtype) for one in weights + m + v),
            in_specs=[pl.BlockSpec(memory_space=pltpu.HBM)] * 12,
            out_specs=(pl.BlockSpec(memory_space=pltpu.VMEM),) * 9,
            scratch_shapes=[pltpu.VMEM(w.shape, kind) for w in weights]
            + [pltpu.VMEM(one.shape, kind) for one in m + m]
            + [pltpu.VMEM((n - 1, plan.tiles, ROWS, LANES), kind), pltpu.VMEM((n, plan.tiles, ROWS, LANES), kind)]
            + [pltpu.SemaphoreType.REGULAR((2,)), dma((3, layers, n - 1)), dma((3,)), dma((3,)), dma((3,))]
            + [dma((3, layers))] * 2
            + [dma((n - 2, len(plan.copies)))] * 2
            + [dma((n - 1, len(plan.copies)))] * 2
            + [dma((2,))] * 2
            + [pltpu.VMEM((AROUND, m[plan.order[0]].shape[2]), kind), dma, dma],
            compiler_params=pltpu.CompilerParams(collective_id=0, has_side_effects=True, vmem_limit_bytes=40 * 2**20),
        )(*arrays)
        new = [pltpu.with_memory_space_constraint(one, pltpu.VMEM) for one in new]
        return pl.pallas_call(
            put,
            out_shape=tuple(pltpu.HBM(one.shape, one.dtype) for one in weights + m + v),
            in_specs=[pl.BlockSpec(memory_space=pltpu.VMEM)] * 9,
            out_specs=(pl.BlockSpec(memory_space=pltpu.HBM),) * 9,
            scratch_shapes=[dma((9,))],
            compiler_params=pltpu.CompilerParams(vmem_limit_bytes=2**20),
        )(*new)

    all_of, part = P(None, None, None), P(None, AXIS, None)
    return jax.shard_map(
        step,
        mesh=mesh,
        in_specs=(P(("rep", AXIS), None, None, None),) * 3 + (all_of,) * 3 + (part,) * 6,
        out_specs=(P("rep", None, None),) * 3 + (P("rep", AXIS, None),) * 6,
        check_vma=False,
    )
```

```python
import functools

import jax
import jax.numpy as jnp
from jax import lax
from jax.experimental import pallas as pl
from jax.experimental.pallas import tpu as pltpu
from jax.sharding import PartitionSpec as P

AXIS = "dp"
MESH = pl.DeviceIdType.MESH
ROWS, LANES = 16, 128
LEFT_OUT = {True: 38, False: 16}
AROUND = 80

def adamw(w, m, v, g):
    m = 0.9 * m + 0.1 * g
    v = 0.95 * v + 0.05 * g * g
    step = m * lax.rsqrt(v + 1e-8) + 0.1 * w
    return (w - 0.02 * step).astype(jnp.bfloat16), m, v

class Plan:
    def __init__(self, shapes):
        self.layers = shapes[0][0]
        self.block = [shape[1] for shape in shapes]
        self.wide = [shape[2] // LANES for shape in shapes]
        half = self.layers // 2
        self.order = sorted(range(len(shapes)), key=lambda i: (self.wide[i], i))
        bands, tile = {}, 0
        for rightward in (False, True):
            bands[rightward] = []
            for layer in range(half) if rightward else range(half, self.layers):
                for i in self.order:
                    for row in range(self.block[i] // ROWS):
                        bands[rightward].append((layer, i, row, tile))
                        tile += self.wide[i]
        self.tiles = tile
        ways = []
        for rightward in (False, True):
            all_of, start = bands[rightward], bands[rightward][0][3]
            at = next(k for k, band in enumerate(all_of) if 2 * (band[3] - start) >= self.tiles // 2)
            ways.append([(rightward, part) for part in (all_of[:at], all_of[at:])])
        self.copies = [
            (rightward, part[0][3], sum(self.wide[i] for _, i, _, _ in part), self.runs(part))
            for pair in zip(*ways, strict=True)
            for rightward, part in pair
        ]

    def runs(self, bands):
        runs = []
        for layer, i, row, tile in bands:
            if runs and runs[-1][:2] == [layer, i]:
                runs[-1][3] += 1
            else:
                runs.append([layer, i, row, 1, tile])
        return runs

def kernel(n, plan, *refs):
    terms, weights, ms, vs = (refs[i : i + 3] for i in (0, 3, 6, 9))
    new_w, new_m, new_v, held, own, first = (refs[i : i + 3] for i in (12, 15, 18, 21, 24, 27))
    around, around_send, around_recv = refs[-3:]
    sums, news, entered, held_sem, own_sem, m_sem, v_sem, first_send, first_recv, sum_send, sum_recv, out_send, out_recv, end_send, end_recv = refs[30:-3]
    me = lax.axis_index(AXIS)
    right, left = lax.rem(me + 1, n), lax.rem(me + n - 1, n)
    half = plan.layers // 2
    every = [(i, layer) for i in plan.order for pair in range(half) for layer in (pair, half + pair)]

    def behind(rightward, steps):
        return lax.rem(me + n - steps if rightward else me + steps, n)

    def rows(i, device):
        return pl.ds(pl.multiple_of(device * plan.block[i], ROWS), plan.block[i])

    def send(rightward, source, target, send_sem, recv_sem):
        return pltpu.make_async_remote_copy(
            src_ref=source,
            dst_ref=target,
            send_sem=send_sem,
            recv_sem=recv_sem,
            device_id={AXIS: right if rightward else left},
            device_id_type=MESH,
        )

    def first_copy(i, layer, skip=0):
        rightward, count = layer < half, plan.block[i] - skip
        source = terms[i].at[0, layer, pl.ds(pl.multiple_of(behind(rightward, 1) * plan.block[i] + skip, ROWS), count)]
        return send(rightward, source, first[i].at[layer, pl.ds(skip, count)], first_send.at[i, layer], first_recv.at[i, layer])

    split = plan.order[0], half
    splits, gets_rest, gets_around = me <= 1, (me == 0) | (me == n - 1), (me == 1) | (me == 2)

    def around_copy():
        i, layer = split
        source = terms[i].at[0, layer, pl.ds(pl.multiple_of(behind(False, 1) * plan.block[i], ROWS), AROUND)]
        return send(True, source, around, around_send, around_recv)

    def either(shorter, short, full, do):
        pl.when(shorter)(lambda: do(short()))
        pl.when(jnp.logical_not(shorter))(lambda: do(full()))

    def first_of(i, layer, shorter, do):
        if (i, layer) == split:
            either(shorter, lambda: first_copy(i, layer, AROUND), lambda: first_copy(i, layer), do)
        else:
            do(first_copy(i, layer))

    def sum_copy(at, step):
        rightward, tile, count, _ = plan.copies[at]
        part = pl.ds(tile, count)
        return send(rightward, sums.at[step - 1, part], sums.at[step, part], sum_send.at[step - 1, at], sum_recv.at[step - 1, at])

    def out_copy(at, step, left_out=0):
        rightward, tile, count, _ = plan.copies[at]
        count -= left_out
        piece = news.at[behind(rightward, step), pl.ds(tile, count)]
        return send(rightward, piece, piece, out_send.at[step, at], out_recv.at[step, at])

    def end_copy(at):
        rightward, tile, count, _ = plan.copies[at]
        piece = news.at[me, pl.ds(tile + count - LEFT_OUT[rightward], LEFT_OUT[rightward])]
        return send(not rightward, piece, piece, end_send.at[int(rightward)], end_recv.at[int(rightward)])

    def load(i, layer, steps):
        part = rows(i, behind(layer < half, steps))
        return pltpu.make_async_copy(terms[i].at[0, layer, part], held[i].at[layer, part], held_sem.at[i, layer, steps - 2])

    def own_load(i):
        return pltpu.make_async_copy(weights[i].at[:, rows(i, me)], own[i], own_sem.at[i])

    def moment_load(i):
        return (pltpu.make_async_copy(ms[i], new_m[i], m_sem.at[i]), pltpu.make_async_copy(vs[i], new_v[i], v_sem.at[i]))

    def each_tile(runs, body, unroll=False):
        for layer, i, row, count, tile in runs:

            @pl.loop(0, count, unroll=unroll)
            def _(k, layer=layer, i=i, row=row, tile=tile):
                for column in range(plan.wide[i]):
                    body(layer, i, (row + k) * ROWS, column * LANES, tile + k * plan.wide[i] + column)

    def tile_of(ref, layer, row, column):
        return ref[layer, pl.ds(pl.multiple_of(row, ROWS), ROWS), pl.ds(column, LANES)]

    def term(i, layer, steps, row, column):
        device = behind(layer < half, steps)
        return tile_of(held[i], layer, device * plan.block[i] + row, column).astype(jnp.float32)

    barrier = pltpu.get_barrier_semaphore()

    @pl.when(me < n - 2)
    def _():
        pl.semaphore_signal(barrier, inc=1, device_id={AXIS: right}, device_id_type=MESH)

    @pl.when((me == 0) | (me == n - 1))
    def _():
        pl.semaphore_signal(barrier, inc=1, device_id={AXIS: left}, device_id_type=MESH)

    def start(rightward):
        for i, layer in every:
            if (layer < half) == rightward:
                first_of(i, layer, splits, lambda copy: copy.start())

    @pl.when(me > 0)
    def _():
        pl.semaphore_wait(barrier, 1 + (me == n - 2).astype(jnp.int32))

    @pl.when((me > 0) & (me < n - 1))
    def _():
        pl.semaphore_signal(entered.at[1], inc=1, device_id={AXIS: left}, device_id_type=MESH)
        start(False)

    @pl.when(me >= n - 2)
    def _():
        pl.semaphore_signal(entered.at[0], inc=1, device_id={AXIS: right}, device_id_type=MESH)
        start(True)

    @pl.when(me < n - 2)
    def _():
        pl.semaphore_wait(entered.at[1], 1)
        start(True)

    @pl.when(splits)
    def _():
        around_copy().start()

    @pl.when((me == 0) | (me == n - 1))
    def _():
        pl.semaphore_wait(entered.at[0], 1)
        start(False)

    @pl.when(gets_rest)
    def _():
        i, layer = split
        first[i][layer, pl.ds(0, AROUND)] = jnp.zeros((AROUND, first[i].shape[2]), first[i].dtype)

    @pl.when(jnp.logical_not(gets_around))
    def _():
        around[...] = jnp.zeros_like(around)

    for steps in range(2, n + 1):
        for i, layer in every:
            load(i, layer, steps).start()
    for i in range(3):
        own_load(i).start()
        for copy in moment_load(i):
            copy.start()

    def wait_loads(runs, steps):
        for layer, i, row, _, _ in runs:
            if row == 0:
                load(i, layer, steps).wait()

    arrived = set()
    for at, (rightward, _, _, runs) in enumerate(plan.copies):
        for layer, i, row, _, _ in runs:
            if (i, layer) not in arrived:
                first_of(i, layer, gets_rest, lambda copy: copy.wait_recv())
                arrived.add((i, layer))
        wait_loads(runs, 2)

        def add_first(layer, i, row, column, tile):
            sums[0, tile] = (tile_of(first[i], layer, row, column).astype(jnp.float32) + term(i, layer, 2, row, column)).astype(jnp.bfloat16)

        each_tile(runs, add_first)
        sum_copy(at, 1).start()

    @pl.loop(1, n - 2)
    def _(step):
        for at, (rightward, _, _, runs) in enumerate(plan.copies):
            sum_copy(at, step).wait_recv()
            wait_loads(runs, step + 2)

            def add(layer, i, row, column, tile):
                sums[step, tile] = (sums[step, tile].astype(jnp.float32) + term(i, layer, step + 2, row, column)).astype(jnp.bfloat16)

            each_tile(runs, add)
            sum_copy(at, step + 1).start()

    for i in range(3):
        own_load(i).wait()
        for copy in moment_load(i):
            copy.wait()

    for at, (rightward, _, _, runs) in enumerate(plan.copies):
        sum_copy(at, n - 2).wait_recv()
        wait_loads(runs, n)

        def take_step(layer, i, row, column, tile, more=None):
            g = sums[n - 2, tile].astype(jnp.float32) + term(i, layer, n, row, column)
            if more is not None:
                g += more[pl.ds(pl.multiple_of(row, ROWS), ROWS), pl.ds(column, LANES)].astype(jnp.float32)
            g = g.astype(jnp.bfloat16).astype(jnp.float32)
            place = (layer, pl.ds(pl.multiple_of(row, ROWS), ROWS), pl.ds(column, LANES))
            w, m, v = adamw(own[i][place].astype(jnp.float32), new_m[i][place], new_v[i][place], g)
            news[me, tile] = w
            new_w[i][layer, pl.ds(pl.multiple_of(me * plan.block[i] + row, ROWS), ROWS), pl.ds(column, LANES)] = w
            new_m[i][place] = m
            new_v[i][place] = v

        for run in runs:
            layer, i, row, count, tile = run
            if (i, layer) == split and row == 0:
                pl.when(gets_around)(lambda: around_copy().wait_recv())
                part = AROUND // ROWS
                each_tile([(layer, i, row, part, tile)], functools.partial(take_step, more=around))
                run = (layer, i, row + part, count - part, tile + part * plan.wide[i])
            each_tile([run], take_step)
        out_copy(at, 0).start()

    for i, layer in every:
        first_of(i, layer, splits, lambda copy: copy.wait_send())
    pl.when(splits)(lambda: around_copy().wait_send())

    def deal(at, step, unroll=False):
        rightward, _, _, runs = plan.copies[at]
        device = behind(rightward, step + 1)

        def move(layer, i, row, column, tile):
            new_w[i][layer, pl.ds(pl.multiple_of(device * plan.block[i] + row, ROWS), ROWS), pl.ds(column, LANES)] = news[device, tile]

        each_tile(runs, move, unroll)

    @pl.loop(0, n - 3)
    def _(step):
        for at in range(len(plan.copies)):
            out_copy(at, step).wait_recv()
            out_copy(at, step + 1).start()
            deal(at, step)
        for at in range(len(plan.copies)):
            sum_copy(at, step + 1).wait_send()

        @pl.when(step > 0)
        def _():
            for at in range(len(plan.copies)):
                out_copy(at, step - 1).wait_send()

    ends = range(len(plan.copies) - 2, len(plan.copies))

    def last(at, shorter, do):
        if at not in ends:
            do(out_copy(at, n - 2))
            return
        left_out = LEFT_OUT[plan.copies[at][0]]
        either(shorter, lambda: out_copy(at, n - 2, left_out), lambda: out_copy(at, n - 2), do)

    def sends_shorter(at):
        return me == (n - 1 if plan.copies[at][0] else 0)

    def gets_shorter(at):
        return me == (0 if plan.copies[at][0] else n - 1)

    def sends_end(at):
        return me == (1 if plan.copies[at][0] else n - 2)

    for at in range(len(plan.copies)):
        out_copy(at, n - 3).wait_recv()
        last(at, sends_shorter(at), lambda copy: copy.start())
        if at in ends:
            pl.when(sends_end(at))(lambda at=at: end_copy(at).start())
        deal(at, n - 3)
    for at in range(len(plan.copies)):
        sum_copy(at, n - 2).wait_send()
        out_copy(at, n - 4).wait_send()
        out_copy(at, n - 3).wait_send()
    for at in range(len(plan.copies)):
        last(at, gets_shorter(at), lambda copy: copy.wait_recv())
        if at in ends:
            pl.when(gets_shorter(at))(lambda at=at: end_copy(at).wait_recv())
        deal(at, n - 2, True)
    for at in range(len(plan.copies)):
        last(at, sends_shorter(at), lambda copy: copy.wait_send())
        if at in ends:
            pl.when(sends_end(at))(lambda at=at: end_copy(at).wait_send())

def put(*refs):
    count = len(refs) // 2
    copies = [pltpu.make_async_copy(refs[i], refs[count + i], refs[-1].at[i]) for i in range(count)]
    for copy in copies:
        copy.start()
    for copy in copies:
        copy.wait()

def solution(mesh):
    n = mesh.shape[AXIS]

    def step(*arrays):
        terms, weights, m, v = (arrays[i : i + 3] for i in (0, 3, 6, 9))
        plan = Plan([one.shape for one in m])
        layers = plan.layers
        dma, kind = pltpu.SemaphoreType.DMA, weights[0].dtype
        arrays = [pltpu.with_memory_space_constraint(one, pltpu.HBM) for one in arrays]
        new = pl.pallas_call(
            functools.partial(kernel, n, plan),
            out_shape=tuple(pltpu.VMEM(one.shape, one.dtype) for one in weights + m + v),
            in_specs=[pl.BlockSpec(memory_space=pltpu.HBM)] * 12,
            out_specs=(pl.BlockSpec(memory_space=pltpu.VMEM),) * 9,
            scratch_shapes=[pltpu.VMEM(w.shape, kind) for w in weights]
            + [pltpu.VMEM(one.shape, kind) for one in m + m]
            + [pltpu.VMEM((n - 1, plan.tiles, ROWS, LANES), kind), pltpu.VMEM((n, plan.tiles, ROWS, LANES), kind)]
            + [pltpu.SemaphoreType.REGULAR((2,)), dma((3, layers, n - 1)), dma((3,)), dma((3,)), dma((3,))]
            + [dma((3, layers))] * 2
            + [dma((n - 2, len(plan.copies)))] * 2
            + [dma((n - 1, len(plan.copies)))] * 2
            + [dma((2,))] * 2
            + [pltpu.VMEM((AROUND, m[plan.order[0]].shape[2]), kind), dma, dma],
            compiler_params=pltpu.CompilerParams(collective_id=0, has_side_effects=True, vmem_limit_bytes=40 * 2**20),
        )(*arrays)
        new = [pltpu.with_memory_space_constraint(one, pltpu.VMEM) for one in new]
        return pl.pallas_call(
            put,
            out_shape=tuple(pltpu.HBM(one.shape, one.dtype) for one in weights + m + v),
            in_specs=[pl.BlockSpec(memory_space=pltpu.VMEM)] * 9,
            out_specs=(pl.BlockSpec(memory_space=pltpu.HBM),) * 9,
            scratch_shapes=[dma((9,))],
            compiler_params=pltpu.CompilerParams(vmem_limit_bytes=2**20),
        )(*new)

    all_of, part = P(None, None, None), P(None, AXIS, None)
    return jax.shard_map(
        step,
        mesh=mesh,
        in_specs=(P(("rep", AXIS), None, None, None),) * 3 + (all_of,) * 3 + (part,) * 6,
        out_specs=(P("rep", None, None),) * 3 + (P("rep", AXIS, None),) * 6,
        check_vma=False,
    )
```

```python
import functools

import jax
import jax.numpy as jnp
from jax import lax
from jax.experimental import pallas as pl
from jax.experimental.pallas import tpu as pltpu
from jax.sharding import PartitionSpec as P

AXIS = "dp"
MESH = pl.DeviceIdType.MESH
ROWS, LANES = 16, 128
LEFT_OUT = {True: 33, False: 16}
AROUND = {True: 48, False: 80}

def adamw(w, m, v, g):
    m = 0.9 * m + 0.1 * g
    v = 0.95 * v + 0.05 * g * g
    step = m * lax.rsqrt(v + 1e-8) + 0.1 * w
    return (w - 0.02 * step).astype(jnp.bfloat16), m, v

class Plan:
    def __init__(self, shapes):
        self.layers = shapes[0][0]
        self.block = [shape[1] for shape in shapes]
        self.wide = [shape[2] // LANES for shape in shapes]
        half = self.layers // 2
        self.order = sorted(range(len(shapes)), key=lambda i: (self.wide[i], i))
        bands, tile = {}, 0
        for rightward in (False, True):
            bands[rightward] = []
            for layer in range(half) if rightward else range(half, self.layers):
                for i in self.order:
                    for row in range(self.block[i] // ROWS):
                        bands[rightward].append((layer, i, row, tile))
                        tile += self.wide[i]
        self.tiles = tile
        ways = []
        for rightward in (False, True):
            all_of, start = bands[rightward], bands[rightward][0][3]
            at = next(k for k, band in enumerate(all_of) if 2 * (band[3] - start) >= self.tiles // 2)
            ways.append([(rightward, part) for part in (all_of[:at], all_of[at:])])
        self.copies = [
            (rightward, part[0][3], sum(self.wide[i] for _, i, _, _ in part), self.runs(part))
            for pair in zip(*ways, strict=True)
            for rightward, part in pair
        ]

    def runs(self, bands):
        runs = []
        for layer, i, row, tile in bands:
            if runs and runs[-1][:2] == [layer, i]:
                runs[-1][3] += 1
            else:
                runs.append([layer, i, row, 1, tile])
        return runs

def kernel(n, plan, *refs):
    terms, weights, ms, vs = (refs[i : i + 3] for i in (0, 3, 6, 9))
    new_w, new_m, new_v, held, own, first = (refs[i : i + 3] for i in (12, 15, 18, 21, 24, 27))
    around, (around_send, around_recv) = {True: refs[-4], False: refs[-3]}, refs[-2:]
    sums, news, entered, held_sem, own_sem, m_sem, v_sem, first_send, first_recv, sum_send, sum_recv, out_send, out_recv, end_send, end_recv = refs[30:-4]
    me = lax.axis_index(AXIS)
    right, left = lax.rem(me + 1, n), lax.rem(me + n - 1, n)
    half = plan.layers // 2
    every = [(i, layer) for i in plan.order for pair in range(half) for layer in (pair, half + pair)]

    def behind(rightward, steps):
        return lax.rem(me + n - steps if rightward else me + steps, n)

    def rows(i, device):
        return pl.ds(pl.multiple_of(device * plan.block[i], ROWS), plan.block[i])

    def send(rightward, source, target, send_sem, recv_sem):
        return pltpu.make_async_remote_copy(
            src_ref=source,
            dst_ref=target,
            send_sem=send_sem,
            recv_sem=recv_sem,
            device_id={AXIS: right if rightward else left},
            device_id_type=MESH,
        )

    def first_copy(i, layer, skip=0):
        rightward, count = layer < half, plan.block[i] - skip
        source = terms[i].at[0, layer, pl.ds(pl.multiple_of(behind(rightward, 1) * plan.block[i] + skip, ROWS), count)]
        return send(rightward, source, first[i].at[layer, pl.ds(skip, count)], first_send.at[i, layer], first_recv.at[i, layer])

    split = {(plan.order[0], 0): True, (plan.order[0], half): False}
    splits = {True: me == n - 1, False: me <= 1}
    gets_rest = {True: me == 0, False: (me == 0) | (me == n - 1)}
    gets_around = {True: me == n - 2, False: (me == 1) | (me == 2)}

    def around_copy(rightward):
        i = plan.order[0]
        part = pl.ds(pl.multiple_of(behind(rightward, 1) * plan.block[i], ROWS), AROUND[rightward])
        source = terms[i].at[0, 0 if rightward else half, part]
        return send(not rightward, source, around[rightward], around_send.at[int(rightward)], around_recv.at[int(rightward)])

    def either(shorter, short, full, do):
        pl.when(shorter)(lambda: do(short()))
        pl.when(jnp.logical_not(shorter))(lambda: do(full()))

    def first_of(i, layer, shorter, do):
        if (i, layer) in split:
            rightward = split[i, layer]
            either(shorter[rightward], lambda: first_copy(i, layer, AROUND[rightward]), lambda: first_copy(i, layer), do)
        else:
            do(first_copy(i, layer))

    def sum_copy(at, step):
        rightward, tile, count, _ = plan.copies[at]
        part = pl.ds(tile, count)
        return send(rightward, sums.at[step - 1, part], sums.at[step, part], sum_send.at[step - 1, at], sum_recv.at[step - 1, at])

    def out_copy(at, step, left_out=0):
        rightward, tile, count, _ = plan.copies[at]
        count -= left_out
        piece = news.at[behind(rightward, step), pl.ds(tile, count)]
        return send(rightward, piece, piece, out_send.at[step, at], out_recv.at[step, at])

    def end_copy(at):
        rightward, tile, count, _ = plan.copies[at]
        piece = news.at[me, pl.ds(tile + count - LEFT_OUT[rightward], LEFT_OUT[rightward])]
        return send(not rightward, piece, piece, end_send.at[int(rightward)], end_recv.at[int(rightward)])

    def load(i, layer, steps):
        part = rows(i, behind(layer < half, steps))
        return pltpu.make_async_copy(terms[i].at[0, layer, part], held[i].at[layer, part], held_sem.at[i, layer, steps - 2])

    def own_load(i):
        return pltpu.make_async_copy(weights[i].at[:, rows(i, me)], own[i], own_sem.at[i])

    def moment_load(i):
        return (pltpu.make_async_copy(ms[i], new_m[i], m_sem.at[i]), pltpu.make_async_copy(vs[i], new_v[i], v_sem.at[i]))

    def each_tile(runs, body, unroll=False):
        for layer, i, row, count, tile in runs:

            @pl.loop(0, count, unroll=unroll)
            def _(k, layer=layer, i=i, row=row, tile=tile):
                for column in range(plan.wide[i]):
                    body(layer, i, (row + k) * ROWS, column * LANES, tile + k * plan.wide[i] + column)

    def tile_of(ref, layer, row, column):
        return ref[layer, pl.ds(pl.multiple_of(row, ROWS), ROWS), pl.ds(column, LANES)]

    def term(i, layer, steps, row, column):
        device = behind(layer < half, steps)
        return tile_of(held[i], layer, device * plan.block[i] + row, column).astype(jnp.float32)

    barrier = pltpu.get_barrier_semaphore()

    @pl.when(me < n - 2)
    def _():
        pl.semaphore_signal(barrier, inc=1, device_id={AXIS: right}, device_id_type=MESH)

    @pl.when((me == 0) | (me == n - 1))
    def _():
        pl.semaphore_signal(barrier, inc=1, device_id={AXIS: left}, device_id_type=MESH)

    def start(rightward):
        for i, layer in every:
            if (layer < half) == rightward:
                first_of(i, layer, splits, lambda copy: copy.start())

    @pl.when(me > 0)
    def _():
        pl.semaphore_wait(barrier, 1 + (me == n - 2).astype(jnp.int32))

    @pl.when((me > 0) & (me < n - 1))
    def _():
        pl.semaphore_signal(entered.at[1], inc=1, device_id={AXIS: left}, device_id_type=MESH)
        start(False)

    @pl.when(me >= n - 2)
    def _():
        pl.semaphore_signal(entered.at[0], inc=1, device_id={AXIS: right}, device_id_type=MESH)
        start(True)

    @pl.when(me < n - 2)
    def _():
        pl.semaphore_wait(entered.at[1], 1)
        start(True)


    @pl.when((me == 0) | (me == n - 1))
    def _():
        pl.semaphore_wait(entered.at[0], 1)
        start(False)

    for (i, layer), rightward in split.items():

        @pl.when(splits[rightward])
        def _(rightward=rightward):
            around_copy(rightward).start()

        @pl.when(gets_rest[rightward])
        def _(i=i, layer=layer, rightward=rightward):
            first[i][layer, pl.ds(0, AROUND[rightward])] = jnp.zeros(around[rightward].shape, first[i].dtype)

        @pl.when(jnp.logical_not(gets_around[rightward]))
        def _(rightward=rightward):
            around[rightward][...] = jnp.zeros_like(around[rightward])

    for steps in range(2, n + 1):
        for i, layer in every:
            load(i, layer, steps).start()
    for i in range(3):
        own_load(i).start()
        for copy in moment_load(i):
            copy.start()

    def wait_loads(runs, steps):
        for layer, i, row, _, _ in runs:
            if row == 0:
                load(i, layer, steps).wait()

    arrived = set()
    for at, (rightward, _, _, runs) in enumerate(plan.copies):
        for layer, i, row, _, _ in runs:
            if (i, layer) not in arrived:
                first_of(i, layer, gets_rest, lambda copy: copy.wait_recv())
                arrived.add((i, layer))
        wait_loads(runs, 2)

        def add_first(layer, i, row, column, tile):
            sums[0, tile] = (tile_of(first[i], layer, row, column).astype(jnp.float32) + term(i, layer, 2, row, column)).astype(jnp.bfloat16)

        each_tile(runs, add_first)
        sum_copy(at, 1).start()

    @pl.loop(1, n - 2)
    def _(step):
        for at, (rightward, _, _, runs) in enumerate(plan.copies):
            sum_copy(at, step).wait_recv()
            wait_loads(runs, step + 2)

            def add(layer, i, row, column, tile):
                sums[step, tile] = (sums[step, tile].astype(jnp.float32) + term(i, layer, step + 2, row, column)).astype(jnp.bfloat16)

            each_tile(runs, add)
            sum_copy(at, step + 1).start()

    for i in range(3):
        own_load(i).wait()
        for copy in moment_load(i):
            copy.wait()

    for at, (rightward, _, _, runs) in enumerate(plan.copies):
        sum_copy(at, n - 2).wait_recv()
        wait_loads(runs, n)

        def take_step(layer, i, row, column, tile, more=None):
            g = sums[n - 2, tile].astype(jnp.float32) + term(i, layer, n, row, column)
            if more is not None:
                g += more[pl.ds(pl.multiple_of(row, ROWS), ROWS), pl.ds(column, LANES)].astype(jnp.float32)
            g = g.astype(jnp.bfloat16).astype(jnp.float32)
            place = (layer, pl.ds(pl.multiple_of(row, ROWS), ROWS), pl.ds(column, LANES))
            w, m, v = adamw(own[i][place].astype(jnp.float32), new_m[i][place], new_v[i][place], g)
            news[me, tile] = w
            new_w[i][layer, pl.ds(pl.multiple_of(me * plan.block[i] + row, ROWS), ROWS), pl.ds(column, LANES)] = w
            new_m[i][place] = m
            new_v[i][place] = v

        for run in runs:
            layer, i, row, count, tile = run
            if (i, layer) in split and row == 0:
                pl.when(gets_around[rightward])(lambda rightward=rightward: around_copy(rightward).wait_recv())
                part = AROUND[rightward] // ROWS
                each_tile([(layer, i, row, part, tile)], functools.partial(take_step, more=around[rightward]))
                run = (layer, i, row + part, count - part, tile + part * plan.wide[i])
            each_tile([run], take_step)
        out_copy(at, 0).start()

    for i, layer in every:
        first_of(i, layer, splits, lambda copy: copy.wait_send())
    for way in (True, False):
        pl.when(splits[way])(lambda way=way: around_copy(way).wait_send())

    def deal(at, step, unroll=False):
        rightward, _, _, runs = plan.copies[at]
        device = behind(rightward, step + 1)

        def move(layer, i, row, column, tile):
            new_w[i][layer, pl.ds(pl.multiple_of(device * plan.block[i] + row, ROWS), ROWS), pl.ds(column, LANES)] = news[device, tile]

        each_tile(runs, move, unroll)

    @pl.loop(0, n - 3)
    def _(step):
        for at in range(len(plan.copies)):
            out_copy(at, step).wait_recv()
            out_copy(at, step + 1).start()
            deal(at, step)
        for at in range(len(plan.copies)):
            sum_copy(at, step + 1).wait_send()

        @pl.when(step > 0)
        def _():
            for at in range(len(plan.copies)):
                out_copy(at, step - 1).wait_send()

    ends = range(len(plan.copies) - 2, len(plan.copies))

    def last(at, shorter, do):
        if at not in ends:
            do(out_copy(at, n - 2))
            return
        left_out = LEFT_OUT[plan.copies[at][0]]
        either(shorter, lambda: out_copy(at, n - 2, left_out), lambda: out_copy(at, n - 2), do)

    def sends_shorter(at):
        return me == (n - 1 if plan.copies[at][0] else 0)

    def gets_shorter(at):
        return me == (0 if plan.copies[at][0] else n - 1)

    def sends_end(at):
        return me == (1 if plan.copies[at][0] else n - 2)

    for at in range(len(plan.copies)):
        out_copy(at, n - 3).wait_recv()
        last(at, sends_shorter(at), lambda copy: copy.start())
        if at in ends:
            pl.when(sends_end(at))(lambda at=at: end_copy(at).start())
        deal(at, n - 3)
    for at in range(len(plan.copies)):
        sum_copy(at, n - 2).wait_send()
        out_copy(at, n - 4).wait_send()
        out_copy(at, n - 3).wait_send()
    for at in range(len(plan.copies)):
        last(at, gets_shorter(at), lambda copy: copy.wait_recv())
        if at in ends:
            pl.when(gets_shorter(at))(lambda at=at: end_copy(at).wait_recv())
        deal(at, n - 2, True)
    for at in range(len(plan.copies)):
        last(at, sends_shorter(at), lambda copy: copy.wait_send())
        if at in ends:
            pl.when(sends_end(at))(lambda at=at: end_copy(at).wait_send())

def put(*refs):
    count = len(refs) // 2
    copies = [pltpu.make_async_copy(refs[i], refs[count + i], refs[-1].at[i]) for i in range(count)]
    for copy in copies:
        copy.start()
    for copy in copies:
        copy.wait()

def solution(mesh):
    n = mesh.shape[AXIS]

    def step(*arrays):
        terms, weights, m, v = (arrays[i : i + 3] for i in (0, 3, 6, 9))
        plan = Plan([one.shape for one in m])
        layers = plan.layers
        dma, kind = pltpu.SemaphoreType.DMA, weights[0].dtype
        arrays = [pltpu.with_memory_space_constraint(one, pltpu.HBM) for one in arrays]
        new = pl.pallas_call(
            functools.partial(kernel, n, plan),
            out_shape=tuple(pltpu.VMEM(one.shape, one.dtype) for one in weights + m + v),
            in_specs=[pl.BlockSpec(memory_space=pltpu.HBM)] * 12,
            out_specs=(pl.BlockSpec(memory_space=pltpu.VMEM),) * 9,
            scratch_shapes=[pltpu.VMEM(w.shape, kind) for w in weights]
            + [pltpu.VMEM(one.shape, kind) for one in m + m]
            + [pltpu.VMEM((n - 1, plan.tiles, ROWS, LANES), kind), pltpu.VMEM((n, plan.tiles, ROWS, LANES), kind)]
            + [pltpu.SemaphoreType.REGULAR((2,)), dma((3, layers, n - 1)), dma((3,)), dma((3,)), dma((3,))]
            + [dma((3, layers))] * 2
            + [dma((n - 2, len(plan.copies)))] * 2
            + [dma((n - 1, len(plan.copies)))] * 2
            + [dma((2,))] * 2
            + [pltpu.VMEM((AROUND[way], m[plan.order[0]].shape[2]), kind) for way in (True, False)]
            + [dma((2,))] * 2,
            compiler_params=pltpu.CompilerParams(collective_id=0, has_side_effects=True, vmem_limit_bytes=40 * 2**20),
        )(*arrays)
        new = [pltpu.with_memory_space_constraint(one, pltpu.VMEM) for one in new]
        return pl.pallas_call(
            put,
            out_shape=tuple(pltpu.HBM(one.shape, one.dtype) for one in weights + m + v),
            in_specs=[pl.BlockSpec(memory_space=pltpu.VMEM)] * 9,
            out_specs=(pl.BlockSpec(memory_space=pltpu.HBM),) * 9,
            scratch_shapes=[dma((9,))],
            compiler_params=pltpu.CompilerParams(vmem_limit_bytes=2**20),
        )(*new)

    all_of, part = P(None, None, None), P(None, AXIS, None)
    return jax.shard_map(
        step,
        mesh=mesh,
        in_specs=(P(("rep", AXIS), None, None, None),) * 3 + (all_of,) * 3 + (part,) * 6,
        out_specs=(P("rep", None, None),) * 3 + (P("rep", AXIS, None),) * 6,
        check_vma=False,
    )
```

```python
import functools

import jax
import jax.numpy as jnp
from jax import lax
from jax.experimental import pallas as pl
from jax.experimental.pallas import tpu as pltpu
from jax.sharding import PartitionSpec as P

AXIS = "dp"
MESH = pl.DeviceIdType.MESH
ROWS, LANES = 16, 128
LEFT_OUT = {True: 28, False: 16}
AROUND = {True: 80, False: 96}

def adamw(w, m, v, g):
    m = 0.9 * m + 0.1 * g
    v = 0.95 * v + 0.05 * g * g
    step = m * lax.rsqrt(v + 1e-8) + 0.1 * w
    return (w - 0.02 * step).astype(jnp.bfloat16), m, v

class Plan:
    def __init__(self, shapes):
        self.layers = shapes[0][0]
        self.block = [shape[1] for shape in shapes]
        self.wide = [shape[2] // LANES for shape in shapes]
        half = self.layers // 2
        self.order = sorted(range(len(shapes)), key=lambda i: (self.wide[i], i))
        bands, tile = {}, 0
        for rightward in (False, True):
            bands[rightward] = []
            for layer in range(half) if rightward else range(half, self.layers):
                for i in self.order:
                    for row in range(self.block[i] // ROWS):
                        bands[rightward].append((layer, i, row, tile))
                        tile += self.wide[i]
        self.tiles = tile
        ways = []
        for rightward in (False, True):
            all_of, start = bands[rightward], bands[rightward][0][3]
            at = next(k for k, band in enumerate(all_of) if 2 * (band[3] - start) >= self.tiles // 2)
            ways.append([(rightward, part) for part in (all_of[:at], all_of[at:])])
        self.copies = [
            (rightward, part[0][3], sum(self.wide[i] for _, i, _, _ in part), self.runs(part))
            for pair in zip(*ways, strict=True)
            for rightward, part in pair
        ]

    def runs(self, bands):
        runs = []
        for layer, i, row, tile in bands:
            if runs and runs[-1][:2] == [layer, i]:
                runs[-1][3] += 1
            else:
                runs.append([layer, i, row, 1, tile])
        return runs

def kernel(n, plan, *refs):
    terms, weights, ms, vs = (refs[i : i + 3] for i in (0, 3, 6, 9))
    new_w, new_m, new_v, held, own, first = (refs[i : i + 3] for i in (12, 15, 18, 21, 24, 27))
    around, (around_send, around_recv) = {True: refs[-4], False: refs[-3]}, refs[-2:]
    sums, news, entered, held_sem, own_sem, m_sem, v_sem, first_send, first_recv, sum_send, sum_recv, out_send, out_recv, end_send, end_recv = refs[30:-4]
    me = lax.axis_index(AXIS)
    right, left = lax.rem(me + 1, n), lax.rem(me + n - 1, n)
    half = plan.layers // 2
    every = [(i, layer) for i in plan.order for pair in range(half) for layer in (pair, half + pair)]

    def behind(rightward, steps):
        return lax.rem(me + n - steps if rightward else me + steps, n)

    def rows(i, device):
        return pl.ds(pl.multiple_of(device * plan.block[i], ROWS), plan.block[i])

    def send(rightward, source, target, send_sem, recv_sem):
        return pltpu.make_async_remote_copy(
            src_ref=source,
            dst_ref=target,
            send_sem=send_sem,
            recv_sem=recv_sem,
            device_id={AXIS: right if rightward else left},
            device_id_type=MESH,
        )

    def first_copy(i, layer, skip=0, loaded=False):
        rightward, count = layer < half, plan.block[i] - skip
        part = pl.ds(pl.multiple_of(behind(rightward, 1) * plan.block[i] + skip, ROWS), count)
        source = held[i].at[layer, part] if loaded else terms[i].at[0, layer, part]
        return send(rightward, source, first[i].at[layer, pl.ds(skip, count)], first_send.at[i, layer], first_recv.at[i, layer])

    split = {(plan.order[0], 0): True, (plan.order[0], half): False}
    splits = {True: me == n - 1, False: me <= 1}
    gets_rest = {True: me == 0, False: (me == 0) | (me == n - 1)}
    gets_around = {True: me == n - 2, False: (me == 1) | (me == 2)}

    def around_copy(rightward):
        i = plan.order[0]
        part = pl.ds(pl.multiple_of(behind(rightward, 1) * plan.block[i], ROWS), AROUND[rightward])
        source = terms[i].at[0, 0 if rightward else half, part]
        return send(not rightward, source, around[rightward], around_send.at[int(rightward)], around_recv.at[int(rightward)])

    def either(shorter, short, full, do):
        pl.when(shorter)(lambda: do(short()))
        pl.when(jnp.logical_not(shorter))(lambda: do(full()))

    def first_of(i, layer, shorter, do, loaded=False):
        if (i, layer) in split:
            rightward = split[i, layer]
            either(shorter[rightward], lambda: first_copy(i, layer, AROUND[rightward], loaded), lambda: first_copy(i, layer, 0, loaded), do)
        else:
            do(first_copy(i, layer, 0, loaded))

    def sum_copy(at, step):
        rightward, tile, count, _ = plan.copies[at]
        part = pl.ds(tile, count)
        return send(rightward, sums.at[step - 1, part], sums.at[step, part], sum_send.at[step - 1, at], sum_recv.at[step - 1, at])

    def out_copy(at, step, left_out=0):
        rightward, tile, count, _ = plan.copies[at]
        count -= left_out
        piece = news.at[behind(rightward, step), pl.ds(tile, count)]
        return send(rightward, piece, piece, out_send.at[step, at], out_recv.at[step, at])

    def end_copy(at):
        rightward, tile, count, _ = plan.copies[at]
        piece = news.at[me, pl.ds(tile + count - LEFT_OUT[rightward], LEFT_OUT[rightward])]
        return send(not rightward, piece, piece, end_send.at[int(rightward)], end_recv.at[int(rightward)])

    def load(i, layer, steps):
        part = rows(i, behind(layer < half, steps))
        return pltpu.make_async_copy(terms[i].at[0, layer, part], held[i].at[layer, part], held_sem.at[i, layer, steps - 1])

    def own_load(i):
        return pltpu.make_async_copy(weights[i].at[:, rows(i, me)], own[i], own_sem.at[i])

    def moment_load(i):
        return (pltpu.make_async_copy(ms[i], new_m[i], m_sem.at[i]), pltpu.make_async_copy(vs[i], new_v[i], v_sem.at[i]))

    def each_tile(runs, body, unroll=False):
        for layer, i, row, count, tile in runs:

            @pl.loop(0, count, unroll=unroll)
            def _(k, layer=layer, i=i, row=row, tile=tile):
                for column in range(plan.wide[i]):
                    body(layer, i, (row + k) * ROWS, column * LANES, tile + k * plan.wide[i] + column)

    def tile_of(ref, layer, row, column):
        return ref[layer, pl.ds(pl.multiple_of(row, ROWS), ROWS), pl.ds(column, LANES)]

    def term(i, layer, steps, row, column):
        device = behind(layer < half, steps)
        return tile_of(held[i], layer, device * plan.block[i] + row, column).astype(jnp.float32)

    barrier = pltpu.get_barrier_semaphore()

    @pl.when(me < n - 2)
    def _():
        pl.semaphore_signal(barrier, inc=1, device_id={AXIS: right}, device_id_type=MESH)

    @pl.when((me == 0) | (me == n - 1))
    def _():
        pl.semaphore_signal(barrier, inc=1, device_id={AXIS: left}, device_id_type=MESH)

    def first_loads(rightward):
        for i, layer in every:
            if (layer < half) == rightward:
                load(i, layer, 1).start()

    def start(rightward, loaded):
        for i, layer in every:
            if (layer < half) == rightward:
                if loaded:
                    load(i, layer, 1).wait()
                first_of(i, layer, splits, lambda copy: copy.start(), loaded)

    inner, ends_of_line = me < n - 2, (me == 0) | (me == n - 1)
    pl.when(inner)(lambda: first_loads(True))
    pl.when(ends_of_line)(lambda: first_loads(False))

    @pl.when(me > 0)
    def _():
        pl.semaphore_wait(barrier, 1 + (me == n - 2).astype(jnp.int32))

    @pl.when((me > 0) & (me < n - 1))
    def _():
        pl.semaphore_signal(entered.at[1], inc=1, device_id={AXIS: left}, device_id_type=MESH)
        start(False, False)

    @pl.when(me >= n - 2)
    def _():
        pl.semaphore_signal(entered.at[0], inc=1, device_id={AXIS: right}, device_id_type=MESH)
        start(True, False)

    @pl.when(inner)
    def _():
        pl.semaphore_wait(entered.at[1], 1)
        start(True, True)

    @pl.when(ends_of_line)
    def _():
        pl.semaphore_wait(entered.at[0], 1)
        start(False, True)

    for (i, layer), rightward in split.items():

        @pl.when(splits[rightward])
        def _(rightward=rightward):
            around_copy(rightward).start()

        @pl.when(gets_rest[rightward])
        def _(i=i, layer=layer, rightward=rightward):
            first[i][layer, pl.ds(0, AROUND[rightward])] = jnp.zeros(around[rightward].shape, first[i].dtype)

        @pl.when(jnp.logical_not(gets_around[rightward]))
        def _(rightward=rightward):
            around[rightward][...] = jnp.zeros_like(around[rightward])

    for steps in range(2, n + 1):
        for i, layer in every:
            load(i, layer, steps).start()
    for i in range(3):
        own_load(i).start()
        for copy in moment_load(i):
            copy.start()

    def wait_loads(runs, steps):
        for layer, i, row, _, _ in runs:
            if row == 0:
                load(i, layer, steps).wait()

    arrived = set()
    for at, (rightward, _, _, runs) in enumerate(plan.copies):
        for layer, i, row, _, _ in runs:
            if (i, layer) not in arrived:
                first_of(i, layer, gets_rest, lambda copy: copy.wait_recv())
                arrived.add((i, layer))
        wait_loads(runs, 2)

        def add_first(layer, i, row, column, tile):
            sums[0, tile] = (tile_of(first[i], layer, row, column).astype(jnp.float32) + term(i, layer, 2, row, column)).astype(jnp.bfloat16)

        each_tile(runs, add_first)
        sum_copy(at, 1).start()

    @pl.loop(1, n - 2)
    def _(step):
        for at, (rightward, _, _, runs) in enumerate(plan.copies):
            sum_copy(at, step).wait_recv()
            wait_loads(runs, step + 2)

            def add(layer, i, row, column, tile):
                sums[step, tile] = (sums[step, tile].astype(jnp.float32) + term(i, layer, step + 2, row, column)).astype(jnp.bfloat16)

            each_tile(runs, add)
            sum_copy(at, step + 1).start()

    for i in range(3):
        own_load(i).wait()
        for copy in moment_load(i):
            copy.wait()

    for at, (rightward, _, _, runs) in enumerate(plan.copies):
        sum_copy(at, n - 2).wait_recv()
        wait_loads(runs, n)

        def take_step(layer, i, row, column, tile, more=None):
            g = sums[n - 2, tile].astype(jnp.float32) + term(i, layer, n, row, column)
            if more is not None:
                g += more[pl.ds(pl.multiple_of(row, ROWS), ROWS), pl.ds(column, LANES)].astype(jnp.float32)
            g = g.astype(jnp.bfloat16).astype(jnp.float32)
            place = (layer, pl.ds(pl.multiple_of(row, ROWS), ROWS), pl.ds(column, LANES))
            w, m, v = adamw(own[i][place].astype(jnp.float32), new_m[i][place], new_v[i][place], g)
            news[me, tile] = w
            new_w[i][layer, pl.ds(pl.multiple_of(me * plan.block[i] + row, ROWS), ROWS), pl.ds(column, LANES)] = w
            new_m[i][place] = m
            new_v[i][place] = v

        for run in runs:
            layer, i, row, count, tile = run
            if (i, layer) in split and row == 0:
                pl.when(gets_around[rightward])(lambda rightward=rightward: around_copy(rightward).wait_recv())
                part = AROUND[rightward] // ROWS
                each_tile([(layer, i, row, part, tile)], functools.partial(take_step, more=around[rightward]))
                run = (layer, i, row + part, count - part, tile + part * plan.wide[i])
            each_tile([run], take_step)
        out_copy(at, 0).start()

    for i, layer in every:
        first_of(i, layer, splits, lambda copy: copy.wait_send())
    for way in (True, False):
        pl.when(splits[way])(lambda way=way: around_copy(way).wait_send())

    def deal(at, step, unroll=False):
        rightward, _, _, runs = plan.copies[at]
        device = behind(rightward, step + 1)

        def move(layer, i, row, column, tile):
            new_w[i][layer, pl.ds(pl.multiple_of(device * plan.block[i] + row, ROWS), ROWS), pl.ds(column, LANES)] = news[device, tile]

        each_tile(runs, move, unroll)

    @pl.loop(0, n - 3)
    def _(step):
        for at in range(len(plan.copies)):
            out_copy(at, step).wait_recv()
            out_copy(at, step + 1).start()
            deal(at, step)
        for at in range(len(plan.copies)):
            sum_copy(at, step + 1).wait_send()

        @pl.when(step > 0)
        def _():
            for at in range(len(plan.copies)):
                out_copy(at, step - 1).wait_send()

    ends = range(len(plan.copies) - 2, len(plan.copies))

    def last(at, shorter, do):
        if at not in ends:
            do(out_copy(at, n - 2))
            return
        left_out = LEFT_OUT[plan.copies[at][0]]
        either(shorter, lambda: out_copy(at, n - 2, left_out), lambda: out_copy(at, n - 2), do)

    def sends_shorter(at):
        return me == (n - 1 if plan.copies[at][0] else 0)

    def gets_shorter(at):
        return me == (0 if plan.copies[at][0] else n - 1)

    def sends_end(at):
        return me == (1 if plan.copies[at][0] else n - 2)

    for at in range(len(plan.copies)):
        out_copy(at, n - 3).wait_recv()
        last(at, sends_shorter(at), lambda copy: copy.start())
        if at in ends:
            pl.when(sends_end(at))(lambda at=at: end_copy(at).start())
        deal(at, n - 3)
    for at in range(len(plan.copies)):
        sum_copy(at, n - 2).wait_send()
        out_copy(at, n - 4).wait_send()
        out_copy(at, n - 3).wait_send()
    for at in range(len(plan.copies)):
        last(at, gets_shorter(at), lambda copy: copy.wait_recv())
        if at in ends:
            pl.when(gets_shorter(at))(lambda at=at: end_copy(at).wait_recv())
        deal(at, n - 2, True)
    for at in range(len(plan.copies)):
        last(at, sends_shorter(at), lambda copy: copy.wait_send())
        if at in ends:
            pl.when(sends_end(at))(lambda at=at: end_copy(at).wait_send())

def put(*refs):
    count = len(refs) // 2
    copies = [pltpu.make_async_copy(refs[i], refs[count + i], refs[-1].at[i]) for i in range(count)]
    for copy in copies:
        copy.start()
    for copy in copies:
        copy.wait()

def solution(mesh):
    n = mesh.shape[AXIS]

    def step(*arrays):
        terms, weights, m, v = (arrays[i : i + 3] for i in (0, 3, 6, 9))
        plan = Plan([one.shape for one in m])
        layers = plan.layers
        dma, kind = pltpu.SemaphoreType.DMA, weights[0].dtype
        arrays = [pltpu.with_memory_space_constraint(one, pltpu.HBM) for one in arrays]
        new = pl.pallas_call(
            functools.partial(kernel, n, plan),
            out_shape=tuple(pltpu.VMEM(one.shape, one.dtype) for one in weights + m + v),
            in_specs=[pl.BlockSpec(memory_space=pltpu.HBM)] * 12,
            out_specs=(pl.BlockSpec(memory_space=pltpu.VMEM),) * 9,
            scratch_shapes=[pltpu.VMEM(w.shape, kind) for w in weights]
            + [pltpu.VMEM(one.shape, kind) for one in m + m]
            + [pltpu.VMEM((n - 1, plan.tiles, ROWS, LANES), kind), pltpu.VMEM((n, plan.tiles, ROWS, LANES), kind)]
            + [pltpu.SemaphoreType.REGULAR((2,)), dma((3, layers, n)), dma((3,)), dma((3,)), dma((3,))]
            + [dma((3, layers))] * 2
            + [dma((n - 2, len(plan.copies)))] * 2
            + [dma((n - 1, len(plan.copies)))] * 2
            + [dma((2,))] * 2
            + [pltpu.VMEM((AROUND[way], m[plan.order[0]].shape[2]), kind) for way in (True, False)]
            + [dma((2,))] * 2,
            compiler_params=pltpu.CompilerParams(collective_id=0, has_side_effects=True, vmem_limit_bytes=40 * 2**20),
        )(*arrays)
        new = [pltpu.with_memory_space_constraint(one, pltpu.VMEM) for one in new]
        return pl.pallas_call(
            put,
            out_shape=tuple(pltpu.HBM(one.shape, one.dtype) for one in weights + m + v),
            in_specs=[pl.BlockSpec(memory_space=pltpu.VMEM)] * 9,
            out_specs=(pl.BlockSpec(memory_space=pltpu.HBM),) * 9,
            scratch_shapes=[dma((9,))],
            compiler_params=pltpu.CompilerParams(vmem_limit_bytes=2**20),
        )(*new)

    all_of, part = P(None, None, None), P(None, AXIS, None)
    return jax.shard_map(
        step,
        mesh=mesh,
        in_specs=(P(("rep", AXIS), None, None, None),) * 3 + (all_of,) * 3 + (part,) * 6,
        out_specs=(P("rep", None, None),) * 3 + (P("rep", AXIS, None),) * 6,
        check_vma=False,
    )
```

```python
import functools

import jax
import jax.numpy as jnp
from jax import lax
from jax.experimental import pallas as pl
from jax.experimental.pallas import tpu as pltpu
from jax.sharding import PartitionSpec as P

AXIS = "dp"
MESH = pl.DeviceIdType.MESH
ROWS, LANES = 16, 128
LEFT_OUT = {True: 28, False: 16}
AROUND = {True: 80, False: 80}

def adamw(w, m, v, g):
    m = 0.9 * m + 0.1 * g
    v = 0.95 * v + 0.05 * g * g
    step = m * lax.rsqrt(v + 1e-8) + 0.1 * w
    return (w - 0.02 * step).astype(jnp.bfloat16), m, v

class Plan:
    def __init__(self, shapes):
        self.layers = shapes[0][0]
        self.block = [shape[1] for shape in shapes]
        self.wide = [shape[2] // LANES for shape in shapes]
        half = self.layers // 2
        self.order = sorted(range(len(shapes)), key=lambda i: (self.wide[i], i))
        bands, tile = {}, 0
        for rightward in (False, True):
            bands[rightward] = []
            for layer in range(half) if rightward else range(half, self.layers):
                for i in self.order:
                    for row in range(self.block[i] // ROWS):
                        bands[rightward].append((layer, i, row, tile))
                        tile += self.wide[i]
        self.tiles = tile
        ways = []
        for rightward in (False, True):
            all_of, start = bands[rightward], bands[rightward][0][3]
            at = next(k for k, band in enumerate(all_of) if 2 * (band[3] - start) >= self.tiles // 2)
            ways.append([(rightward, part) for part in (all_of[:at], all_of[at:])])
        self.copies = [
            (rightward, part[0][3], sum(self.wide[i] for _, i, _, _ in part), self.runs(part))
            for pair in zip(*ways, strict=True)
            for rightward, part in pair
        ]

    def runs(self, bands):
        runs = []
        for layer, i, row, tile in bands:
            if runs and runs[-1][:2] == [layer, i]:
                runs[-1][3] += 1
            else:
                runs.append([layer, i, row, 1, tile])
        return runs

def kernel(n, plan, *refs):
    terms, weights, ms, vs = (refs[i : i + 3] for i in (0, 3, 6, 9))
    new_w, new_m, new_v, held, own, first = (refs[i : i + 3] for i in (12, 15, 18, 21, 24, 27))
    around, (around_send, around_recv) = {True: refs[-4], False: refs[-3]}, refs[-2:]
    sums, news, entered, held_sem, own_sem, m_sem, v_sem, first_send, first_recv, sum_send, sum_recv, out_send, out_recv, end_send, end_recv = refs[30:-4]
    me = lax.axis_index(AXIS)
    right, left = lax.rem(me + 1, n), lax.rem(me + n - 1, n)
    half = plan.layers // 2
    every = [(i, layer) for i in plan.order for pair in range(half) for layer in (pair, half + pair)]

    def behind(rightward, steps):
        return lax.rem(me + n - steps if rightward else me + steps, n)

    def rows(i, device):
        return pl.ds(pl.multiple_of(device * plan.block[i], ROWS), plan.block[i])

    def send(rightward, source, target, send_sem, recv_sem):
        return pltpu.make_async_remote_copy(
            src_ref=source,
            dst_ref=target,
            send_sem=send_sem,
            recv_sem=recv_sem,
            device_id={AXIS: right if rightward else left},
            device_id_type=MESH,
        )

    def first_copy(i, layer, skip=0):
        rightward, count = layer < half, plan.block[i] - skip
        source = terms[i].at[0, layer, pl.ds(pl.multiple_of(behind(rightward, 1) * plan.block[i] + skip, ROWS), count)]
        return send(rightward, source, first[i].at[layer, pl.ds(skip, count)], first_send.at[i, layer], first_recv.at[i, layer])

    split = {(plan.order[0], 0): True, (plan.order[0], half): False}
    splits = {True: me == n - 1, False: me <= 1}
    gets_rest = {True: me == 0, False: (me == 0) | (me == n - 1)}
    gets_around = {True: me == n - 2, False: (me == 1) | (me == 2)}

    def around_copy(rightward):
        i = plan.order[0]
        part = pl.ds(pl.multiple_of(behind(rightward, 1) * plan.block[i], ROWS), AROUND[rightward])
        source = terms[i].at[0, 0 if rightward else half, part]
        return send(not rightward, source, around[rightward], around_send.at[int(rightward)], around_recv.at[int(rightward)])

    def either(shorter, short, full, do):
        pl.when(shorter)(lambda: do(short()))
        pl.when(jnp.logical_not(shorter))(lambda: do(full()))

    def first_of(i, layer, shorter, do):
        if (i, layer) in split:
            rightward = split[i, layer]
            either(shorter[rightward], lambda: first_copy(i, layer, AROUND[rightward]), lambda: first_copy(i, layer), do)
        else:
            do(first_copy(i, layer))

    def sum_copy(at, step):
        rightward, tile, count, _ = plan.copies[at]
        part = pl.ds(tile, count)
        return send(rightward, sums.at[step - 1, part], sums.at[step, part], sum_send.at[step - 1, at], sum_recv.at[step - 1, at])

    def out_copy(at, step, left_out=0):
        rightward, tile, count, _ = plan.copies[at]
        count -= left_out
        piece = news.at[behind(rightward, step), pl.ds(tile, count)]
        return send(rightward, piece, piece, out_send.at[step, at], out_recv.at[step, at])

    def end_copy(at):
        rightward, tile, count, _ = plan.copies[at]
        piece = news.at[me, pl.ds(tile + count - LEFT_OUT[rightward], LEFT_OUT[rightward])]
        return send(not rightward, piece, piece, end_send.at[int(rightward)], end_recv.at[int(rightward)])

    def load(i, layer, steps):
        part = rows(i, behind(layer < half, steps))
        return pltpu.make_async_copy(terms[i].at[0, layer, part], held[i].at[layer, part], held_sem.at[i, layer, steps - 2])

    def own_load(i):
        return pltpu.make_async_copy(weights[i].at[:, rows(i, me)], own[i], own_sem.at[i])

    def moment_load(i):
        return (pltpu.make_async_copy(ms[i], new_m[i], m_sem.at[i]), pltpu.make_async_copy(vs[i], new_v[i], v_sem.at[i]))

    def each_tile(runs, body, unroll=False):
        for layer, i, row, count, tile in runs:

            @pl.loop(0, count, unroll=unroll)
            def _(k, layer=layer, i=i, row=row, tile=tile):
                for column in range(plan.wide[i]):
                    body(layer, i, (row + k) * ROWS, column * LANES, tile + k * plan.wide[i] + column)

    def tile_of(ref, layer, row, column):
        return ref[layer, pl.ds(pl.multiple_of(row, ROWS), ROWS), pl.ds(column, LANES)]

    def term(i, layer, steps, row, column):
        device = behind(layer < half, steps)
        return tile_of(held[i], layer, device * plan.block[i] + row, column).astype(jnp.float32)

    barrier = pltpu.get_barrier_semaphore()

    @pl.when(me < n - 2)
    def _():
        pl.semaphore_signal(barrier, inc=1, device_id={AXIS: right}, device_id_type=MESH)

    @pl.when((me == 0) | (me == n - 1))
    def _():
        pl.semaphore_signal(barrier, inc=1, device_id={AXIS: left}, device_id_type=MESH)

    def start(rightward):
        for i, layer in every:
            if (layer < half) == rightward:
                first_of(i, layer, splits, lambda copy: copy.start())

    @pl.when(me > 0)
    def _():
        pl.semaphore_wait(barrier, 1 + (me == n - 2).astype(jnp.int32))

    @pl.when((me > 0) & (me < n - 1))
    def _():
        pl.semaphore_signal(entered.at[1], inc=1, device_id={AXIS: left}, device_id_type=MESH)
        start(False)

    @pl.when(me >= n - 2)
    def _():
        pl.semaphore_signal(entered.at[0], inc=1, device_id={AXIS: right}, device_id_type=MESH)
        start(True)

    @pl.when(me < n - 2)
    def _():
        pl.semaphore_wait(entered.at[1], 1)
        start(True)


    @pl.when((me == 0) | (me == n - 1))
    def _():
        pl.semaphore_wait(entered.at[0], 1)
        start(False)

    for (i, layer), rightward in split.items():

        @pl.when(splits[rightward])
        def _(rightward=rightward):
            around_copy(rightward).start()

        @pl.when(gets_rest[rightward])
        def _(i=i, layer=layer, rightward=rightward):
            first[i][layer, pl.ds(0, AROUND[rightward])] = jnp.zeros(around[rightward].shape, first[i].dtype)

        @pl.when(jnp.logical_not(gets_around[rightward]))
        def _(rightward=rightward):
            around[rightward][...] = jnp.zeros_like(around[rightward])

    for steps in range(2, n + 1):
        for i, layer in every:
            load(i, layer, steps).start()
    for i in range(3):
        own_load(i).start()
        for copy in moment_load(i):
            copy.start()

    def wait_loads(runs, steps):
        for layer, i, row, _, _ in runs:
            if row == 0:
                load(i, layer, steps).wait()

    arrived = set()
    for at, (rightward, _, _, runs) in enumerate(plan.copies):
        for layer, i, row, _, _ in runs:
            if (i, layer) not in arrived:
                first_of(i, layer, gets_rest, lambda copy: copy.wait_recv())
                arrived.add((i, layer))
        wait_loads(runs, 2)

        def add_first(layer, i, row, column, tile):
            sums[0, tile] = (tile_of(first[i], layer, row, column).astype(jnp.float32) + term(i, layer, 2, row, column)).astype(jnp.bfloat16)

        each_tile(runs, add_first)
        sum_copy(at, 1).start()

    @pl.loop(1, n - 2)
    def _(step):
        for at, (rightward, _, _, runs) in enumerate(plan.copies):
            sum_copy(at, step).wait_recv()
            wait_loads(runs, step + 2)

            def add(layer, i, row, column, tile):
                sums[step, tile] = (sums[step, tile].astype(jnp.float32) + term(i, layer, step + 2, row, column)).astype(jnp.bfloat16)

            each_tile(runs, add)
            sum_copy(at, step + 1).start()

    for i in range(3):
        own_load(i).wait()
        for copy in moment_load(i):
            copy.wait()

    for at, (rightward, _, _, runs) in enumerate(plan.copies):
        sum_copy(at, n - 2).wait_recv()
        wait_loads(runs, n)

        def take_step(layer, i, row, column, tile, more=None):
            g = sums[n - 2, tile].astype(jnp.float32) + term(i, layer, n, row, column)
            if more is not None:
                g += more[pl.ds(pl.multiple_of(row, ROWS), ROWS), pl.ds(column, LANES)].astype(jnp.float32)
            g = g.astype(jnp.bfloat16).astype(jnp.float32)
            place = (layer, pl.ds(pl.multiple_of(row, ROWS), ROWS), pl.ds(column, LANES))
            w, m, v = adamw(own[i][place].astype(jnp.float32), new_m[i][place], new_v[i][place], g)
            news[me, tile] = w
            new_w[i][layer, pl.ds(pl.multiple_of(me * plan.block[i] + row, ROWS), ROWS), pl.ds(column, LANES)] = w
            new_m[i][place] = m
            new_v[i][place] = v

        for run in runs:
            layer, i, row, count, tile = run
            if (i, layer) in split and row == 0:
                pl.when(gets_around[rightward])(lambda rightward=rightward: around_copy(rightward).wait_recv())
                part = AROUND[rightward] // ROWS
                each_tile([(layer, i, row, part, tile)], functools.partial(take_step, more=around[rightward]))
                run = (layer, i, row + part, count - part, tile + part * plan.wide[i])
            each_tile([run], take_step)
        out_copy(at, 0).start()

    for i, layer in every:
        first_of(i, layer, splits, lambda copy: copy.wait_send())
    for way in (True, False):
        pl.when(splits[way])(lambda way=way: around_copy(way).wait_send())

    def deal(at, step, unroll=False):
        rightward, _, _, runs = plan.copies[at]
        device = behind(rightward, step + 1)

        def move(layer, i, row, column, tile):
            new_w[i][layer, pl.ds(pl.multiple_of(device * plan.block[i] + row, ROWS), ROWS), pl.ds(column, LANES)] = news[device, tile]

        each_tile(runs, move, unroll)

    @pl.loop(0, n - 3)
    def _(step):
        for at in range(len(plan.copies)):
            out_copy(at, step).wait_recv()
            out_copy(at, step + 1).start()
            deal(at, step)
        for at in range(len(plan.copies)):
            sum_copy(at, step + 1).wait_send()

        @pl.when(step > 0)
        def _():
            for at in range(len(plan.copies)):
                out_copy(at, step - 1).wait_send()

    ends = range(len(plan.copies) - 2, len(plan.copies))

    def last(at, shorter, do):
        if at not in ends:
            do(out_copy(at, n - 2))
            return
        left_out = LEFT_OUT[plan.copies[at][0]]
        either(shorter, lambda: out_copy(at, n - 2, left_out), lambda: out_copy(at, n - 2), do)

    def sends_shorter(at):
        return me == n - 1 if plan.copies[at][0] else (me == 0) | (me == n - 1)

    def gets_shorter(at):
        return me == 0 if plan.copies[at][0] else (me == n - 1) | (me == n - 2)

    def sends_end(at):
        return me == 1 if plan.copies[at][0] else (me == n - 2) | (me == n - 3)

    for at in range(len(plan.copies)):
        out_copy(at, n - 3).wait_recv()
        last(at, sends_shorter(at), lambda copy: copy.start())
        if at in ends:
            pl.when(sends_end(at))(lambda at=at: end_copy(at).start())
        deal(at, n - 3)
    for at in range(len(plan.copies)):
        sum_copy(at, n - 2).wait_send()
        out_copy(at, n - 4).wait_send()
        out_copy(at, n - 3).wait_send()
    for at in range(len(plan.copies)):
        last(at, gets_shorter(at), lambda copy: copy.wait_recv())
        if at in ends:
            pl.when(gets_shorter(at))(lambda at=at: end_copy(at).wait_recv())
        deal(at, n - 2, True)
    for at in range(len(plan.copies)):
        last(at, sends_shorter(at), lambda copy: copy.wait_send())
        if at in ends:
            pl.when(sends_end(at))(lambda at=at: end_copy(at).wait_send())

def put(*refs):
    count = len(refs) // 2
    copies = [pltpu.make_async_copy(refs[i], refs[count + i], refs[-1].at[i]) for i in range(count)]
    for i, copy in enumerate(copies):
        copy.start(priority=i % 2)
    for copy in copies:
        copy.wait()

def solution(mesh):
    n = mesh.shape[AXIS]

    def step(*arrays):
        terms, weights, m, v = (arrays[i : i + 3] for i in (0, 3, 6, 9))
        plan = Plan([one.shape for one in m])
        layers = plan.layers
        dma, kind = pltpu.SemaphoreType.DMA, weights[0].dtype
        arrays = [pltpu.with_memory_space_constraint(one, pltpu.HBM) for one in arrays]
        new = pl.pallas_call(
            functools.partial(kernel, n, plan),
            out_shape=tuple(pltpu.VMEM(one.shape, one.dtype) for one in weights + m + v),
            in_specs=[pl.BlockSpec(memory_space=pltpu.HBM)] * 12,
            out_specs=(pl.BlockSpec(memory_space=pltpu.VMEM),) * 9,
            scratch_shapes=[pltpu.VMEM(w.shape, kind) for w in weights]
            + [pltpu.VMEM(one.shape, kind) for one in m + m]
            + [pltpu.VMEM((n - 1, plan.tiles, ROWS, LANES), kind), pltpu.VMEM((n, plan.tiles, ROWS, LANES), kind)]
            + [pltpu.SemaphoreType.REGULAR((2,)), dma((3, layers, n - 1)), dma((3,)), dma((3,)), dma((3,))]
            + [dma((3, layers))] * 2
            + [dma((n - 2, len(plan.copies)))] * 2
            + [dma((n - 1, len(plan.copies)))] * 2
            + [dma((2,))] * 2
            + [pltpu.VMEM((AROUND[way], m[plan.order[0]].shape[2]), kind) for way in (True, False)]
            + [dma((2,))] * 2,
            compiler_params=pltpu.CompilerParams(collective_id=0, has_side_effects=True, vmem_limit_bytes=40 * 2**20),
        )(*arrays)
        new = [pltpu.with_memory_space_constraint(one, pltpu.VMEM) for one in new]
        return pl.pallas_call(
            put,
            out_shape=tuple(pltpu.HBM(one.shape, one.dtype) for one in weights + m + v),
            in_specs=[pl.BlockSpec(memory_space=pltpu.VMEM)] * 9,
            out_specs=(pl.BlockSpec(memory_space=pltpu.HBM),) * 9,
            scratch_shapes=[dma((9,))],
            compiler_params=pltpu.CompilerParams(vmem_limit_bytes=2**20),
        )(*new)

    all_of, part = P(None, None, None), P(None, AXIS, None)
    return jax.shard_map(
        step,
        mesh=mesh,
        in_specs=(P(("rep", AXIS), None, None, None),) * 3 + (all_of,) * 3 + (part,) * 6,
        out_specs=(P("rep", None, None),) * 3 + (P("rep", AXIS, None),) * 6,
        check_vma=False,
    )
```

```python
import functools

import jax
import jax.numpy as jnp
from jax import lax
from jax.experimental import pallas as pl
from jax.experimental.pallas import tpu as pltpu
from jax.sharding import PartitionSpec as P

AXIS = "dp"
MESH = pl.DeviceIdType.MESH
ROWS, LANES = 16, 128
LEFT_OUT = {True: 28, False: 11}
AROUND = {True: 80, False: 80}

def adamw(w, m, v, g):
    m = 0.9 * m + 0.1 * g
    v = 0.95 * v + 0.05 * g * g
    step = m * lax.rsqrt(v + 1e-8) + 0.1 * w
    return (w - 0.02 * step).astype(jnp.bfloat16), m, v

class Plan:
    def __init__(self, shapes):
        self.layers = shapes[0][0]
        self.block = [shape[1] for shape in shapes]
        self.wide = [shape[2] // LANES for shape in shapes]
        half = self.layers // 2
        self.order = sorted(range(len(shapes)), key=lambda i: (self.wide[i], i))
        bands, tile = {}, 0
        for rightward in (False, True):
            bands[rightward] = []
            for layer in range(half) if rightward else range(half, self.layers):
                for i in self.order:
                    for row in range(self.block[i] // ROWS):
                        bands[rightward].append((layer, i, row, tile))
                        tile += self.wide[i]
        self.tiles = tile
        ways = []
        for rightward in (False, True):
            all_of, start = bands[rightward], bands[rightward][0][3]
            at = next(k for k, band in enumerate(all_of) if 2 * (band[3] - start) >= self.tiles // 2)
            ways.append([(rightward, part) for part in (all_of[:at], all_of[at:])])
        self.copies = [
            (rightward, part[0][3], sum(self.wide[i] for _, i, _, _ in part), self.runs(part))
            for pair in zip(*ways, strict=True)
            for rightward, part in pair
        ]

    def runs(self, bands):
        runs = []
        for layer, i, row, tile in bands:
            if runs and runs[-1][:2] == [layer, i]:
                runs[-1][3] += 1
            else:
                runs.append([layer, i, row, 1, tile])
        return runs

def kernel(n, plan, *refs):
    terms, weights, ms, vs = (refs[i : i + 3] for i in (0, 3, 6, 9))
    new_w, new_m, new_v, held, own, first = (refs[i : i + 3] for i in (12, 15, 18, 21, 24, 27))
    around, (around_send, around_recv) = {True: refs[-4], False: refs[-3]}, refs[-2:]
    sums, news, entered, held_sem, own_sem, m_sem, v_sem, first_send, first_recv, sum_send, sum_recv, out_send, out_recv, end_send, end_recv = refs[30:-4]
    me = lax.axis_index(AXIS)
    right, left = lax.rem(me + 1, n), lax.rem(me + n - 1, n)
    half = plan.layers // 2
    every = [(i, layer) for i in plan.order for pair in range(half) for layer in (pair, half + pair)]

    def behind(rightward, steps):
        return lax.rem(me + n - steps if rightward else me + steps, n)

    def rows(i, device):
        return pl.ds(pl.multiple_of(device * plan.block[i], ROWS), plan.block[i])

    def send(rightward, source, target, send_sem, recv_sem):
        return pltpu.make_async_remote_copy(
            src_ref=source,
            dst_ref=target,
            send_sem=send_sem,
            recv_sem=recv_sem,
            device_id={AXIS: right if rightward else left},
            device_id_type=MESH,
        )

    def first_copy(i, layer, skip=0):
        rightward, count = layer < half, plan.block[i] - skip
        source = terms[i].at[0, layer, pl.ds(pl.multiple_of(behind(rightward, 1) * plan.block[i] + skip, ROWS), count)]
        return send(rightward, source, first[i].at[layer, pl.ds(skip, count)], first_send.at[i, layer], first_recv.at[i, layer])

    split = {(plan.order[0], 0): True, (plan.order[0], half): False}
    splits = {True: me == n - 1, False: me <= 1}
    gets_rest = {True: me == 0, False: (me == 0) | (me == n - 1)}
    gets_around = {True: me == n - 2, False: (me == 1) | (me == 2)}

    def around_copy(rightward):
        i = plan.order[0]
        part = pl.ds(pl.multiple_of(behind(rightward, 1) * plan.block[i], ROWS), AROUND[rightward])
        source = terms[i].at[0, 0 if rightward else half, part]
        return send(not rightward, source, around[rightward], around_send.at[int(rightward)], around_recv.at[int(rightward)])

    def either(shorter, short, full, do):
        pl.when(shorter)(lambda: do(short()))
        pl.when(jnp.logical_not(shorter))(lambda: do(full()))

    def first_of(i, layer, shorter, do):
        if (i, layer) in split:
            rightward = split[i, layer]
            either(shorter[rightward], lambda: first_copy(i, layer, AROUND[rightward]), lambda: first_copy(i, layer), do)
        else:
            do(first_copy(i, layer))

    def sum_copy(at, step):
        rightward, tile, count, _ = plan.copies[at]
        part = pl.ds(tile, count)
        return send(rightward, sums.at[step - 1, part], sums.at[step, part], sum_send.at[step - 1, at], sum_recv.at[step - 1, at])

    def out_copy(at, step, left_out=0):
        rightward, tile, count, _ = plan.copies[at]
        count -= left_out
        piece = news.at[behind(rightward, step), pl.ds(tile, count)]
        return send(rightward, piece, piece, out_send.at[step, at], out_recv.at[step, at])

    def end_copy(at):
        rightward, tile, count, _ = plan.copies[at]
        piece = news.at[me, pl.ds(tile + count - LEFT_OUT[rightward], LEFT_OUT[rightward])]
        return send(not rightward, piece, piece, end_send.at[int(rightward)], end_recv.at[int(rightward)])

    def load(i, layer, steps):
        part = rows(i, behind(layer < half, steps))
        return pltpu.make_async_copy(terms[i].at[0, layer, part], held[i].at[layer, part], held_sem.at[i, layer, steps - 2])

    def own_load(i):
        return pltpu.make_async_copy(weights[i].at[:, rows(i, me)], own[i], own_sem.at[i])

    def moment_load(i):
        return (pltpu.make_async_copy(ms[i], new_m[i], m_sem.at[i]), pltpu.make_async_copy(vs[i], new_v[i], v_sem.at[i]))

    def each_tile(runs, body, unroll=False):
        for layer, i, row, count, tile in runs:

            @pl.loop(0, count, unroll=unroll)
            def _(k, layer=layer, i=i, row=row, tile=tile):
                for column in range(plan.wide[i]):
                    body(layer, i, (row + k) * ROWS, column * LANES, tile + k * plan.wide[i] + column)

    def tile_of(ref, layer, row, column):
        return ref[layer, pl.ds(pl.multiple_of(row, ROWS), ROWS), pl.ds(column, LANES)]

    def term(i, layer, steps, row, column):
        device = behind(layer < half, steps)
        return tile_of(held[i], layer, device * plan.block[i] + row, column).astype(jnp.float32)

    barrier = pltpu.get_barrier_semaphore()

    @pl.when(me < n - 2)
    def _():
        pl.semaphore_signal(barrier, inc=1, device_id={AXIS: right}, device_id_type=MESH)

    @pl.when((me == 0) | (me == n - 1))
    def _():
        pl.semaphore_signal(barrier, inc=1, device_id={AXIS: left}, device_id_type=MESH)

    def start(rightward):
        for i, layer in every:
            if (layer < half) == rightward:
                first_of(i, layer, splits, lambda copy: copy.start())

    @pl.when(me > 0)
    def _():
        pl.semaphore_wait(barrier, 1 + (me == n - 2).astype(jnp.int32))

    @pl.when((me > 0) & (me < n - 1))
    def _():
        pl.semaphore_signal(entered.at[1], inc=1, device_id={AXIS: left}, device_id_type=MESH)
        start(False)

    @pl.when(me >= n - 2)
    def _():
        pl.semaphore_signal(entered.at[0], inc=1, device_id={AXIS: right}, device_id_type=MESH)
        start(True)

    @pl.when(me < n - 2)
    def _():
        pl.semaphore_wait(entered.at[1], 1)
        start(True)


    @pl.when((me == 0) | (me == n - 1))
    def _():
        pl.semaphore_wait(entered.at[0], 1)
        start(False)

    for (i, layer), rightward in split.items():

        @pl.when(splits[rightward])
        def _(rightward=rightward):
            around_copy(rightward).start()

        @pl.when(gets_rest[rightward])
        def _(i=i, layer=layer, rightward=rightward):
            first[i][layer, pl.ds(0, AROUND[rightward])] = jnp.zeros(around[rightward].shape, first[i].dtype)

        @pl.when(jnp.logical_not(gets_around[rightward]))
        def _(rightward=rightward):
            around[rightward][...] = jnp.zeros_like(around[rightward])

    for steps in range(2, n + 1):
        for i, layer in every:
            load(i, layer, steps).start()
    for i in range(3):
        own_load(i).start()
        for copy in moment_load(i):
            copy.start()

    def wait_loads(runs, steps):
        for layer, i, row, _, _ in runs:
            if row == 0:
                load(i, layer, steps).wait()

    arrived = set()
    for at, (rightward, _, _, runs) in enumerate(plan.copies):
        for layer, i, row, _, _ in runs:
            if (i, layer) not in arrived:
                first_of(i, layer, gets_rest, lambda copy: copy.wait_recv())
                arrived.add((i, layer))
        wait_loads(runs, 2)

        def add_first(layer, i, row, column, tile):
            sums[0, tile] = (tile_of(first[i], layer, row, column).astype(jnp.float32) + term(i, layer, 2, row, column)).astype(jnp.bfloat16)

        each_tile(runs, add_first)
        sum_copy(at, 1).start()

    @pl.loop(1, n - 2)
    def _(step):
        for at, (rightward, _, _, runs) in enumerate(plan.copies):
            sum_copy(at, step).wait_recv()
            wait_loads(runs, step + 2)

            def add(layer, i, row, column, tile):
                sums[step, tile] = (sums[step, tile].astype(jnp.float32) + term(i, layer, step + 2, row, column)).astype(jnp.bfloat16)

            each_tile(runs, add)
            sum_copy(at, step + 1).start()

    for i in range(3):
        own_load(i).wait()
        for copy in moment_load(i):
            copy.wait()

    for at, (rightward, _, _, runs) in enumerate(plan.copies):
        sum_copy(at, n - 2).wait_recv()
        wait_loads(runs, n)

        def take_step(layer, i, row, column, tile, more=None):
            g = sums[n - 2, tile].astype(jnp.float32) + term(i, layer, n, row, column)
            if more is not None:
                g += more[pl.ds(pl.multiple_of(row, ROWS), ROWS), pl.ds(column, LANES)].astype(jnp.float32)
            g = g.astype(jnp.bfloat16).astype(jnp.float32)
            place = (layer, pl.ds(pl.multiple_of(row, ROWS), ROWS), pl.ds(column, LANES))
            w, m, v = adamw(own[i][place].astype(jnp.float32), new_m[i][place], new_v[i][place], g)
            news[me, tile] = w
            new_w[i][layer, pl.ds(pl.multiple_of(me * plan.block[i] + row, ROWS), ROWS), pl.ds(column, LANES)] = w
            new_m[i][place] = m
            new_v[i][place] = v

        for run in runs:
            layer, i, row, count, tile = run
            if (i, layer) in split and row == 0:
                pl.when(gets_around[rightward])(lambda rightward=rightward: around_copy(rightward).wait_recv())
                part = AROUND[rightward] // ROWS
                each_tile([(layer, i, row, part, tile)], functools.partial(take_step, more=around[rightward]))
                run = (layer, i, row + part, count - part, tile + part * plan.wide[i])
            each_tile([run], take_step)
        out_copy(at, 0).start()

    for i, layer in every:
        first_of(i, layer, splits, lambda copy: copy.wait_send())
    for way in (True, False):
        pl.when(splits[way])(lambda way=way: around_copy(way).wait_send())

    def deal(at, step, unroll=False):
        rightward, _, _, runs = plan.copies[at]
        device = behind(rightward, step + 1)

        def move(layer, i, row, column, tile):
            new_w[i][layer, pl.ds(pl.multiple_of(device * plan.block[i] + row, ROWS), ROWS), pl.ds(column, LANES)] = news[device, tile]

        each_tile(runs, move, unroll)

    @pl.loop(0, n - 3)
    def _(step):
        for at in range(len(plan.copies)):
            out_copy(at, step).wait_recv()
            out_copy(at, step + 1).start()
            deal(at, step)
        for at in range(len(plan.copies)):
            sum_copy(at, step + 1).wait_send()

        @pl.when(step > 0)
        def _():
            for at in range(len(plan.copies)):
                out_copy(at, step - 1).wait_send()

    ends = range(len(plan.copies) - 2, len(plan.copies))

    def last(at, shorter, do):
        if at not in ends:
            do(out_copy(at, n - 2))
            return
        left_out = LEFT_OUT[plan.copies[at][0]]
        either(shorter, lambda: out_copy(at, n - 2, left_out), lambda: out_copy(at, n - 2), do)

    def sends_shorter(at):
        return me == n - 1 if plan.copies[at][0] else (me == 0) | (me == n - 1)

    def gets_shorter(at):
        return me == 0 if plan.copies[at][0] else (me == n - 1) | (me == n - 2)

    def sends_end(at):
        return me == 1 if plan.copies[at][0] else (me == n - 2) | (me == n - 3)

    for at in range(len(plan.copies)):
        out_copy(at, n - 3).wait_recv()
        last(at, sends_shorter(at), lambda copy: copy.start())
        if at in ends:
            pl.when(sends_end(at))(lambda at=at: end_copy(at).start())
        deal(at, n - 3)
    for at in range(len(plan.copies)):
        sum_copy(at, n - 2).wait_send()
        out_copy(at, n - 4).wait_send()
        out_copy(at, n - 3).wait_send()
    for at in range(len(plan.copies)):
        last(at, gets_shorter(at), lambda copy: copy.wait_recv())
        if at in ends:
            pl.when(gets_shorter(at))(lambda at=at: end_copy(at).wait_recv())
        deal(at, n - 2, True)
    for at in range(len(plan.copies)):
        last(at, sends_shorter(at), lambda copy: copy.wait_send())
        if at in ends:
            pl.when(sends_end(at))(lambda at=at: end_copy(at).wait_send())

def put(*refs):
    count = len(refs) // 2
    copies = [pltpu.make_async_copy(refs[i], refs[count + i], refs[-1].at[i]) for i in range(count)]
    for copy in copies:
        copy.start()
    for copy in copies:
        copy.wait()

def solution(mesh):
    n = mesh.shape[AXIS]

    def step(*arrays):
        terms, weights, m, v = (arrays[i : i + 3] for i in (0, 3, 6, 9))
        plan = Plan([one.shape for one in m])
        layers = plan.layers
        dma, kind = pltpu.SemaphoreType.DMA, weights[0].dtype
        arrays = [pltpu.with_memory_space_constraint(one, pltpu.HBM) for one in arrays]
        new = pl.pallas_call(
            functools.partial(kernel, n, plan),
            out_shape=tuple(pltpu.VMEM(one.shape, one.dtype) for one in weights + m + v),
            in_specs=[pl.BlockSpec(memory_space=pltpu.HBM)] * 12,
            out_specs=(pl.BlockSpec(memory_space=pltpu.VMEM),) * 9,
            scratch_shapes=[pltpu.VMEM(w.shape, kind) for w in weights]
            + [pltpu.VMEM(one.shape, kind) for one in m + m]
            + [pltpu.VMEM((n - 1, plan.tiles, ROWS, LANES), kind), pltpu.VMEM((n, plan.tiles, ROWS, LANES), kind)]
            + [pltpu.SemaphoreType.REGULAR((2,)), dma((3, layers, n - 1)), dma((3,)), dma((3,)), dma((3,))]
            + [dma((3, layers))] * 2
            + [dma((n - 2, len(plan.copies)))] * 2
            + [dma((n - 1, len(plan.copies)))] * 2
            + [dma((2,))] * 2
            + [pltpu.VMEM((AROUND[way], m[plan.order[0]].shape[2]), kind) for way in (True, False)]
            + [dma((2,))] * 2,
            compiler_params=pltpu.CompilerParams(collective_id=0, has_side_effects=True, vmem_limit_bytes=40 * 2**20),
        )(*arrays)
        new = [pltpu.with_memory_space_constraint(one, pltpu.VMEM) for one in new]
        return pl.pallas_call(
            put,
            out_shape=tuple(pltpu.HBM(one.shape, one.dtype) for one in weights + m + v),
            in_specs=[pl.BlockSpec(memory_space=pltpu.VMEM)] * 9,
            out_specs=(pl.BlockSpec(memory_space=pltpu.HBM),) * 9,
            scratch_shapes=[dma((9,))],
            compiler_params=pltpu.CompilerParams(vmem_limit_bytes=2**20),
        )(*new)

    all_of, part = P(None, None, None), P(None, AXIS, None)
    return jax.shard_map(
        step,
        mesh=mesh,
        in_specs=(P(("rep", AXIS), None, None, None),) * 3 + (all_of,) * 3 + (part,) * 6,
        out_specs=(P("rep", None, None),) * 3 + (P("rep", AXIS, None),) * 6,
        check_vma=False,
    )
```
